32 devices in a mesh: rep: 2 (over x), px: 4 (over y, core), py: 4 (over z).
Axes of the slice: x: 2, y: 2, z: 4, core: 2. Of those that a mesh axis runs over, the one named last changes fastest.
Arguments:
- density: float32 [4, 128, 128, 128], P('rep', 'px', 'py'), parts along dimension 0, may hold values from -6 to 6
- kernel_factors: float32 [3, 89, 256], replicated, as said below
Outputs:
- potential: float32 [4, 128, 128, 128], P('rep', 'px', 'py'), parts along dimension 0
The draws below stay inside these ranges and needn't reach their ends.
There are 2 independent parts, one for each index of `rep`. The reference program is written for one: setup_inputs(seed, part) draws one part's arguments, and reference() takes and returns one part's arrays. A program takes and returns all parts, laid end to end along the dimension named above; an argument that names none is the same for every part. Nothing has to cross between parts.
Inputs may be any that keep to these rules, and one draw needn't show every extreme that they name: Each factor is even in its frequency, kernel_factors[d, g, k] = kernel_factors[d, g, 256 - k], and is zero at k = 128.
All inputs are finite; a program needn't handle non-finite values.
Results may differ from the reference program's by a relative error of at most 0.00005.
Values sent between devices are 32-bit elements; how exact they have to be, the bound alone decides.
A program may use at most 128 MiB of HBM per device.

```python
import math
import jax
import jax.numpy as jnp
from jax import lax

N = 128
G = 89
B = 2
M = 256


def draw_kernel_factors(key, part):
    first_key, second_key = jax.random.split(jax.random.fold_in(key, 7))
    widths = jnp.exp(jax.random.uniform(first_key, (G,), jnp.float32, math.log(0.05), math.log(50.0)))
    weights = 20.0 / G * jnp.exp(jax.random.uniform(second_key, (G,), jnp.float32, math.log(0.5), math.log(2.0)))
    frequency = jnp.arange(M, dtype=jnp.int32)
    wrapped = jnp.minimum(frequency, M - frequency).astype(jnp.float32)
    argument = (2.0 * math.pi * wrapped / M) ** 2
    inside = (wrapped < N).astype(jnp.float32)
    base = jnp.exp(-widths[:, None] * argument[None, :]) * inside[None, :]
    return jnp.stack([base * weights[:, None], base, base], 0).astype(jnp.float32)


def levels(stream_key, extent, cuts, smallest, high):
    gain, own = 1.0, jax.random.fold_in(stream_key, 6)
    for dim, blocks in cuts:
        draws = jnp.exp(jax.random.uniform(jax.random.fold_in(own, dim), (blocks,), jnp.float32, smallest / len(cuts), high / len(cuts)))
        gain = gain * jnp.repeat(draws, extent[dim] // blocks).reshape([-1 if axis == dim else 1 for axis in range(len(extent))])
    return gain


def centred(key, shape, spread, most, pieces=(), held_as=jnp.bfloat16):
    level = levels(key, shape, pieces, -0.22, 0.18) if pieces else 1.0
    entries = jax.random.normal(key, shape, jnp.float32) * spread * level
    return jnp.minimum(jnp.maximum(entries, -most), most).astype(held_as)


def setup_inputs(seed: int = 0, part: int = 0) -> dict:
    key_of = jax.random.split(jax.random.key(seed), 3)
    part_splits = jax.random.split(jax.random.fold_in(key_of[2], part), 3)
    return {
        "density": centred(part_splits[0], (B, N, N, N), 1.0, 6.0, ((1, 4), (2, 4)), jnp.float32),
        "kernel_factors": draw_kernel_factors(jax.random.fold_in(key_of[2], 71), part),
    }


def reference(density, kernel_factors):
    highest = lax.Precision.HIGHEST
    plane_xy = kernel_factors[0][:, :, None] * kernel_factors[1][:, None, :]
    kernel = jnp.einsum("gxy,gz->xyz", plane_xy, kernel_factors[2], precision=highest)

    def solve_one(replica):
        padded = jnp.pad(replica, ((0, M - N), (0, M - N), (0, M - N)))
        spectrum = jnp.fft.fftn(padded)
        potential_field = jnp.fft.ifftn(spectrum * kernel).real
        return potential_field[:N, :N, :N].astype(jnp.float32)

    return lax.map(solve_one, density)
```

```python
import math

import jax
import jax.numpy as jnp
import numpy as np
from jax import lax
from jax.experimental import pallas as pl
from jax.experimental.pallas import tpu as pltpu
from jax.sharding import PartitionSpec as P

HIGHEST = lax.Precision.HIGHEST
LANES = 128
TILES = 4
PITCH = 136


def spectral_table(length, chunks):
    freq = np.arange(length).reshape(chunks, 1, length // chunks, 1)
    angle = (freq * np.arange(length) % (2 * length)) * (math.pi / length)
    both = np.concatenate([np.cos(angle), np.sin(angle)], 1)
    return both.reshape(2 * length, length).astype(np.float32)


def dot(spec, left, right):
    return jnp.einsum(spec, left, right, precision=HIGHEST, preferred_element_type=jnp.float32)


def kernel_block(factors, y_start, y_count, z_start, z_count):
    length = factors.shape[2] // 2
    weights = np.full((length,), 1.0 / length, np.float32)
    weights[0] = 0.5 / length
    factors = factors[:, :, :length] * weights
    factor_y = lax.dynamic_slice_in_dim(factors[1], y_start, y_count, 1)
    factor_z = lax.dynamic_slice_in_dim(factors[2], z_start, z_count, 1)
    pair = factor_z[:, :, None] * factor_y[:, None, :]
    return jnp.einsum("gzy,gx->zyx", pair, factors[0], precision=lax.Precision.HIGHEST)


def plain_body(density, kernel_factors):
    replicas, rows_x, rows_y, length = density.shape
    count_px = lax.axis_size("px")
    count_py = lax.axis_size("py")
    half = count_px // replicas
    trade = [[i + half * r for r in range(replicas)] for i in range(half)]
    lines = [[r * half + i for i in range(half)] for r in range(replicas)]
    index_x = lax.axis_index("px") % half
    index_y = lax.axis_index("py")
    table_z = spectral_table(length, count_py)
    table_y = spectral_table(length, half)
    order = np.arange(length).reshape(replicas, half, rows_x).transpose(1, 0, 2).reshape(-1)
    table_x = spectral_table(length, 1)[:, order]

    held = lax.all_to_all(density, "px", 0, 0, axis_index_groups=trade, tiled=True)
    held = held.reshape(replicas * rows_x, rows_y, length)
    held = dot("kz,xyz->kyx", table_z, held)
    held = lax.all_to_all(held, "py", 0, 1, tiled=True)
    held = dot("qy,kyx->kqx", table_y, held)
    held = lax.all_to_all(held, "px", 1, 2, axis_index_groups=lines, tiled=True)
    z_freq, y_freq = length // count_py, length // half
    kernel = kernel_block(kernel_factors, index_x * y_freq, y_freq, index_y * z_freq, z_freq)
    held = dot("kqx,px->kqp", held, table_x)
    held = held.reshape(2, z_freq, 2, y_freq, 2, length) * kernel[None, :, None, :, None, :]
    held = held.reshape(2 * z_freq, 2 * y_freq, 2 * length)
    held = dot("kqp,px->kqx", held, table_x)
    held = lax.all_to_all(held, "px", 2, 1, axis_index_groups=lines, tiled=True)
    held = dot("kqx,qy->kyx", held, table_y)
    held = lax.all_to_all(held, "py", 1, 0, tiled=True)
    held = dot("kyx,kz->xyz", held, table_z)
    held = held.reshape(replicas, rows_x, rows_y, length)
    return lax.all_to_all(held, "px", 0, 0, axis_index_groups=trade, tiled=True)


def halves(values):
    high = values.astype(jnp.bfloat16)
    low = (values - high.astype(jnp.float32)).astype(jnp.bfloat16)
    return high, low


def matmul(left, right):
    return lax.dot_general(left, right, (((1,), (0,)), ((), ())), preferred_element_type=jnp.float32)


def sector_kernel(
    dens, factors, fold_z, fold_y, wide, tall, back_tall, back_wide, open_y, open_z, out,
    a, z, b, p, swap, x, e, kern, keep, c_send, c_held, g, g_send, zr, fin,
    flat, turned, gains,
    sems_z, sems_y, sems_c, sems_ci, sems_yi, sems_zi,
):
    replicas, rows_x, rows_y, length = dens.shape
    half = length // 2
    tiles = rows_x // 2
    chunks = tiles // TILES
    me_px, me_py = lax.axis_index("px"), lax.axis_index("py")
    count_px, count_py = lax.axis_size("px"), lax.axis_size("py")
    side, core = lax.div(me_px, 2), lax.rem(me_px, 2)
    sign = 2 * side - 1
    part = side * (me_px - 2) + (1 - side) * (1 - me_px)
    peers = {1: me_py + 1 - 2 * lax.rem(me_py, 2), 2: lax.rem(me_py + 2, count_py), 3: count_py - 1 - me_py}

    def role(py):
        return 1 - lax.div(lax.rem(py + 1, count_py), 2), lax.div(py, 2)

    mine, odd_z = role(me_py)
    outer = mine == 1
    twin = count_px - 1 - me_px
    other = me_px + 1 - 2 * core
    started = []

    def make(src, dst, sems, slot, device):
        return pltpu.make_async_remote_copy(
            src_ref=src, dst_ref=dst, send_sem=sems.at[(0,) + slot], recv_sem=sems.at[(1,) + slot],
            device_id=device, device_id_type=pl.DeviceIdType.MESH,
        )

    def span(chunk):
        return pl.ds(chunk * TILES, TILES)

    def lines(py):
        return pl.ds(pl.multiple_of(py * rows_y, 8), rows_y)

    def row(tile):
        return side * tile + (1 - side) * (rows_x - 1 - tile)

    def fold(replica, chunk):
        left = [dens[replica, row(chunk * TILES + i)] for i in range(TILES)]
        right = [dens[replica, row(tiles + chunk * TILES + i)] for i in range(TILES)]
        both = jnp.concatenate([jnp.concatenate(left, 0), jnp.concatenate(right, 0)], 1)
        waves = matmul(jnp.concatenate(halves(both), 1), fold_z[...])
        for parity in range(2):
            cut = waves[:, parity * length : (parity + 1) * length]
            a[replica, parity, span(chunk)] = cut.reshape(TILES, rows_y, length)

    sends_z = {}
    for chunk in range(chunks):
        for step, peer in peers.items():
            replica, parity = role(peer)
            sends_z[step, chunk] = make(
                a.at[replica, parity, span(chunk)], z.at[span(chunk), lines(me_py), :],
                sems_z, (step, chunk), {"py": peer},
            )
    for replica in range(replicas):
        for chunk in range(chunks):
            fold(replica, chunk)

            @pl.when(outer)
            def _(replica=replica, chunk=chunk):
                for step in ((2, 1) if replica == 0 else (3,)):
                    sends_z[step, chunk].start()

            @pl.when(jnp.logical_not(outer))
            def _(replica=replica, chunk=chunk):
                for step in ((3,) if replica == 0 else (2, 1)):
                    sends_z[step, chunk].start()

    @pl.loop(0, tiles, unroll=4)
    def _(tile):
        z[tile, lines(me_py), :] = a[mine, odd_z, tile]

    terms = factors.shape[1]
    flat[...] = jnp.zeros_like(flat)
    where = lax.broadcasted_iota(jnp.int32, (terms, length), 1)
    weight = jnp.where(where == 0, 0.5 / length, 1.0 / length)
    for dim in range(3):
        flat[dim, 0:terms] = factors[dim, :, 0:length] * weight
    for dim in range(2):
        turned[dim] = flat[dim].T
    high, low = halves(flat[2])
    gains[...] = jnp.concatenate(
        [jnp.concatenate([high, low], 1), jnp.concatenate([high, jnp.zeros_like(low)], 1)], 0
    )

    @pl.loop(0, length, unroll=4)
    def _(f):
        pair = turned[0] * turned[1, pl.ds(f, 1), :]
        sums = matmul(jnp.concatenate(halves(pair), 1), gains[...])
        kern[f] = sums[:, :length] + sums[:, length:]

    sends_y, sends_c = [], []

    def fold_lines(chunk):
        for step in peers:
            sends_z[step, chunk].wait_recv()
        for i in range(0, TILES, 2):
            tile = chunk * TILES + i
            cells = jnp.concatenate([z[tile], z[tile + 1]], 1)
            waves = matmul(fold_y[...], jnp.concatenate(halves(cells), 0))
            for parity in range(2):
                for j in range(2):
                    b[parity, tile + j] = waves[
                        parity * half : (parity + 1) * half, j * length : (j + 1) * length
                    ]
        copy = make(b.at[1 - side, span(chunk)], p.at[span(chunk)], sems_y, (chunk,), {"px": twin})
        copy.start()
        sends_y.append(copy)

    flip = sign.astype(jnp.float32)
    is_odd = core.astype(jnp.float32)
    even_or = (1.0 - is_odd) + is_odd * flip
    odd_or = (1.0 - is_odd) * flip + is_odd

    def fold_sheets(chunk):
        sends_y[chunk].wait_recv()
        for i in range(TILES):
            tile = chunk * TILES + i
            ours, theirs = b[side, tile], p[tile]
            total, gap = ours + theirs, (ours - theirs) * flip
            x[part, tile] = jnp.where(core == 0, total, gap)
            swap[tile] = jnp.where(core == 0, gap, total)
        copy = make(swap.at[span(chunk)], x.at[part, span(chunk)], sems_c, (chunk,), {"px": other})
        copy.start()
        sends_c.append(copy)

    def forward(chunk):
        sends_c[chunk].wait_recv()

        @pl.loop(0, 2)
        def _(where):
            cells = x[where, span(chunk)].reshape(TILES * half, length)
            high, low = halves(cells)
            waves = matmul(jnp.concatenate([high, low, high], 1), wide[odd_z])
            for i in range(TILES):
                high, low = halves(waves[i * half : (i + 1) * half])
                both = matmul(tall[side], jnp.concatenate([high, high, low], 0))
                for j in range(2):
                    start = (where * rows_x + j * tiles + chunk * TILES + i) * PITCH
                    e[pl.ds(pl.multiple_of(start, 8), length), :] = both[:, j * length : (j + 1) * length]

    for stage in range(chunks + 2):
        if stage < chunks:
            fold_lines(stage)
        if 0 <= stage - 1 < chunks:
            fold_sheets(stage - 1)
        if 0 <= stage - 2:
            forward(stage - 2)

    @pl.loop(0, length // 2, unroll=2)
    def _(f):
        cells = jnp.concatenate([e[pl.ds(2 * f + i, half, stride=PITCH), :] for i in range(2)], 1)
        high, low = halves(cells)
        waves = matmul(tall[core], jnp.concatenate([high, high, low], 0))
        product = waves * jnp.concatenate([kern[2 * f], kern[2 * f + 1]], 1)
        cells = matmul(back_tall[core], jnp.concatenate(halves(product), 0))
        cells = cells[:half] + cells[half:]
        for i in range(2):
            e[pl.ds(2 * f + i, half, stride=PITCH), :] = cells[:, i * length : (i + 1) * length]

    sends_ci, sends_yi, sends_zi = [], [], {}

    def backward(chunk):
        for where in (1 - part, part):
            found = []
            for i in range(TILES):
                cells = []
                for j in range(2):
                    start = (where * rows_x + j * tiles + chunk * TILES + i) * PITCH
                    cells.append(e[pl.ds(pl.multiple_of(start, 8), length), :])
                cells = matmul(
                    back_tall[side], jnp.concatenate(halves(jnp.concatenate(cells, 1)), 0)
                )
                found.append(cells[:half] + cells[half:])
            high, low = halves(jnp.concatenate(found, 0))
            cells = matmul(jnp.concatenate([high, low, high], 1), back_wide[odd_z])
            cells = cells.reshape(TILES, half, length)
            if where is part:
                keep[span(chunk)] = cells
            else:
                c_send[span(chunk)] = cells
                copy = make(
                    c_send.at[span(chunk)], c_held.at[span(chunk)], sems_ci, (chunk,), {"px": other}
                )
                copy.start()
                sends_ci.append(copy)

    def open_sheets(chunk):
        sends_ci[chunk].wait_recv()
        for i in range(TILES):
            tile = chunk * TILES + i
            first, second = keep[tile], c_held[tile]
            even = jnp.where(core == 0, first, second)
            odd = jnp.where(core == 0, second, first) * flip
            g[side, tile] = even + odd
            g_send[tile] = even - odd
        copy = make(
            g_send.at[span(chunk)], g.at[side, span(chunk)], sems_yi, (chunk,), {"px": twin}
        )
        copy.start()
        sends_yi.append(copy)

    def open_lines(chunk):
        sends_yi[chunk].wait_recv()
        for i in range(0, TILES, 2):
            tile = chunk * TILES + i
            both = [
                jnp.concatenate([g[parity, tile], g[parity, tile + 1]], 1) for parity in range(2)
            ]
            cells = matmul(open_y[...], jnp.concatenate(halves(jnp.concatenate(both, 0)), 0))
            for j in range(2):
                zr[tile + j] = cells[:, j * length : (j + 1) * length]
        for step in (3, 2, 1):
            copy = make(
                zr.at[span(chunk), lines(peers[step]), :], fin.at[mine, odd_z, span(chunk)],
                sems_zi, (step, chunk), {"py": peers[step]},
            )
            copy.start()
            sends_zi[step, chunk] = copy
        fin[mine, odd_z, span(chunk)] = zr[span(chunk), lines(me_py), :]

    for stage in range(chunks + 2):
        if stage < chunks:
            backward(stage)
        if 0 <= stage - 1 < chunks:
            open_sheets(stage - 1)
        if 0 <= stage - 2:
            open_lines(stage - 2)

    for replica in range(replicas):
        for chunk in range(chunks):

            @pl.when(outer)
            def _(replica=replica, chunk=chunk):
                for step in ((2, 1) if replica == 0 else (3,)):
                    sends_zi[step, chunk].wait_recv()

            @pl.when(jnp.logical_not(outer))
            def _(replica=replica, chunk=chunk):
                for step in ((3,) if replica == 0 else (2, 1)):
                    sends_zi[step, chunk].wait_recv()

            both = [
                fin[replica, parity, span(chunk)].reshape(TILES * rows_y, length) for parity in range(2)
            ]
            cells = matmul(
                jnp.concatenate(halves(jnp.concatenate(both, 1)), 1), open_z[...]
            )
            for i in range(TILES):
                cut = cells[i * rows_y : (i + 1) * rows_y]
                tile = chunk * TILES + i
                out[replica, row(tile)] = cut[:, :length]
                out[replica, row(tiles + tile)] = cut[:, length:]

    for copy in [*sends_z.values(), *sends_y, *sends_c, *sends_ci, *sends_yi, *sends_zi.values()]:
        copy.wait_send()


def twice(table):
    zero = np.zeros_like(table)
    return np.block([[table, zero], [zero, table]])


def tables_of(length):
    half = length // 2
    angle = (np.arange(length)[:, None] * (2 * np.arange(half) + 1) % (4 * length)) * (math.pi / (2 * length))
    waves = np.stack([np.cos(angle), np.sin(angle)]).astype(np.float32)
    high = waves.astype(jnp.bfloat16).astype(np.float32)
    low = waves - high
    near, far = np.eye(half), np.eye(half)[::-1]
    line = np.block([[far, near], [-far, near]])
    sides = [line[:half].T, line[half:].T]
    fold_z = np.concatenate([twice(side) for side in sides], 1)
    fold_z = np.concatenate([fold_z, fold_z], 0)
    fold_y = np.concatenate([line, line], 1)
    open_y = np.concatenate([line.T, line.T], 1)
    open_z = np.concatenate([twice(side.T) for side in sides], 0)
    open_z = np.concatenate([open_z, open_z], 0)
    wide, tall, back_tall, back_wide = [], [], [], []
    for parity in range(2):
        up, down = high[parity], low[parity]
        wide.append(np.concatenate([twice(up.T), twice(up.T), twice(down.T)], 0))
        tall.append(np.concatenate([up, down, up], 1))
        back_tall.append(np.block([[up.T, up.T], [down.T, np.zeros_like(down.T)]]))
        back_wide.append(np.concatenate([twice(up), twice(up), twice(down)], 0))
    found = (fold_z, fold_y, np.stack(wide), np.stack(tall), np.stack(back_tall), np.stack(back_wide), open_y, open_z)
    return [jnp.asarray(table.astype(np.float32).astype(jnp.bfloat16)) for table in found]


def sector_body(density, kernel_factors):
    replicas, rows_x, rows_y, length = density.shape
    half, tiles = length // 2, rows_x // 2
    chunks = tiles // TILES
    count_px, count_py = lax.axis_size("px"), lax.axis_size("py")
    f32, bf16 = jnp.float32, jnp.bfloat16
    dma = pltpu.SemaphoreType.DMA
    sheet = (tiles, half, length)
    return pl.pallas_call(
        sector_kernel,
        out_shape=jax.ShapeDtypeStruct(density.shape, f32),
        in_specs=[pl.BlockSpec(memory_space=pltpu.VMEM)] * 10,
        out_specs=pl.BlockSpec(memory_space=pltpu.VMEM),
        scratch_shapes=[
            pltpu.VMEM((replicas, 2, tiles, rows_y, length), f32),
            pltpu.VMEM((tiles, length, length), f32),
            pltpu.VMEM((2,) + sheet, f32), pltpu.VMEM(sheet, f32), pltpu.VMEM(sheet, f32),
            pltpu.VMEM((2,) + sheet, f32),
            pltpu.VMEM((half * PITCH, length), f32),
            pltpu.VMEM((length, length, length), f32),
            pltpu.VMEM(sheet, f32), pltpu.VMEM(sheet, f32), pltpu.VMEM(sheet, f32),
            pltpu.VMEM((2,) + sheet, f32), pltpu.VMEM(sheet, f32),
            pltpu.VMEM((tiles, length, length), f32),
            pltpu.VMEM((replicas, 2, tiles, rows_y, length), f32),
            pltpu.VMEM((3, length, length), f32), pltpu.VMEM((2, length, length), f32),
            pltpu.VMEM((2 * length, 2 * length), bf16),
            dma((2, count_py, chunks)), dma((2, chunks)), dma((2, chunks)),
            dma((2, chunks)), dma((2, chunks)), dma((2, count_py, chunks)),
        ],
        compiler_params=pltpu.CompilerParams(has_side_effects=True, vmem_limit_bytes=56 * 2**20),
    )(density, kernel_factors, *tables_of(length))


def body(density, kernel_factors):
    replicas, rows_x, rows_y, length = density.shape
    count_px, count_py = lax.axis_size("px"), lax.axis_size("py")
    square = count_px == count_py == 2 * replicas == 4
    whole = rows_x * count_px == rows_y * count_py == length == LANES
    if square and whole and kernel_factors.shape[1] <= LANES:
        return sector_body(density, kernel_factors)
    return plain_body(density, kernel_factors)


def solution(mesh):
    placed = (P("rep", "px", "py", None), P())
    return jax.shard_map(
        body, mesh=mesh, in_specs=placed, out_specs=P("rep", "px", "py", None), check_vma=False
    )
```

```python
import math

import jax
import jax.numpy as jnp
import numpy as np
from jax import lax
from jax.experimental import pallas as pl
from jax.experimental.pallas import tpu as pltpu
from jax.sharding import PartitionSpec as P

HIGHEST = lax.Precision.HIGHEST
LANES = 128
TILES = 2
LAG = 2
PITCH = 136


def spectral_table(length, chunks):
    freq = np.arange(length).reshape(chunks, 1, length // chunks, 1)
    angle = (freq * np.arange(length) % (2 * length)) * (math.pi / length)
    both = np.concatenate([np.cos(angle), np.sin(angle)], 1)
    return both.reshape(2 * length, length).astype(np.float32)


def dot(spec, left, right):
    return jnp.einsum(spec, left, right, precision=HIGHEST, preferred_element_type=jnp.float32)


def kernel_block(factors, y_start, y_count, z_start, z_count):
    length = factors.shape[2] // 2
    weights = np.full((length,), 1.0 / length, np.float32)
    weights[0] = 0.5 / length
    factors = factors[:, :, :length] * weights
    factor_y = lax.dynamic_slice_in_dim(factors[1], y_start, y_count, 1)
    factor_z = lax.dynamic_slice_in_dim(factors[2], z_start, z_count, 1)
    pair = factor_z[:, :, None] * factor_y[:, None, :]
    return jnp.einsum("gzy,gx->zyx", pair, factors[0], precision=lax.Precision.HIGHEST)


def plain_body(density, kernel_factors):
    replicas, rows_x, rows_y, length = density.shape
    count_px = lax.axis_size("px")
    count_py = lax.axis_size("py")
    half = count_px // replicas
    trade = [[i + half * r for r in range(replicas)] for i in range(half)]
    lines = [[r * half + i for i in range(half)] for r in range(replicas)]
    index_x = lax.axis_index("px") % half
    index_y = lax.axis_index("py")
    table_z = spectral_table(length, count_py)
    table_y = spectral_table(length, half)
    order = np.arange(length).reshape(replicas, half, rows_x).transpose(1, 0, 2).reshape(-1)
    table_x = spectral_table(length, 1)[:, order]

    held = lax.all_to_all(density, "px", 0, 0, axis_index_groups=trade, tiled=True)
    held = held.reshape(replicas * rows_x, rows_y, length)
    held = dot("kz,xyz->kyx", table_z, held)
    held = lax.all_to_all(held, "py", 0, 1, tiled=True)
    held = dot("qy,kyx->kqx", table_y, held)
    held = lax.all_to_all(held, "px", 1, 2, axis_index_groups=lines, tiled=True)
    z_freq, y_freq = length // count_py, length // half
    kernel = kernel_block(kernel_factors, index_x * y_freq, y_freq, index_y * z_freq, z_freq)
    held = dot("kqx,px->kqp", held, table_x)
    held = held.reshape(2, z_freq, 2, y_freq, 2, length) * kernel[None, :, None, :, None, :]
    held = held.reshape(2 * z_freq, 2 * y_freq, 2 * length)
    held = dot("kqp,px->kqx", held, table_x)
    held = lax.all_to_all(held, "px", 2, 1, axis_index_groups=lines, tiled=True)
    held = dot("kqx,qy->kyx", held, table_y)
    held = lax.all_to_all(held, "py", 1, 0, tiled=True)
    held = dot("kyx,kz->xyz", held, table_z)
    held = held.reshape(replicas, rows_x, rows_y, length)
    return lax.all_to_all(held, "px", 0, 0, axis_index_groups=trade, tiled=True)


def halves(values):
    high = values.astype(jnp.bfloat16)
    low = (values - high.astype(jnp.float32)).astype(jnp.bfloat16)
    return high, low


def matmul(left, right):
    return lax.dot_general(left, right, (((1,), (0,)), ((), ())), preferred_element_type=jnp.float32)


def sector_kernel(
    dens_in, factors_in, fold_z_in, fold_y_in, wide_in, tall_in, back_tall_in, back_wide_in, open_y_in, open_z_in, out,
    dens, factors, fold_z, fold_y, wide, tall, back_tall, back_wide, open_y, open_z,
    a, z, b, p, swap, x, e, turned_e, kern, keep, c_send, c_held, g, g_send, zr, fin, found,
    flat, turned, gains,
    sems_z, sems_y, sems_c, sems_ci, sems_yi, sems_zi, sems_in, sems_out,
):
    replicas, rows_x, rows_y, length = dens.shape
    half = length // 2
    tiles = rows_x // 2
    chunks = tiles // TILES
    me_px, me_py = lax.axis_index("px"), lax.axis_index("py")
    count_px, count_py = lax.axis_size("px"), lax.axis_size("py")
    side, core = lax.div(me_px, 2), lax.rem(me_px, 2)
    sign = 2 * side - 1
    part = side * (me_px - 2) + (1 - side) * (1 - me_px)
    peers = {1: me_py + 1 - 2 * lax.rem(me_py, 2), 2: lax.rem(me_py + 2, count_py), 3: count_py - 1 - me_py}

    def role(py):
        return lax.div(lax.rem(py + 1, count_py), 2), lax.div(py, 2)

    mine, odd_z = role(me_py)
    outer = mine == 0
    twin = count_px - 1 - me_px
    other = me_px + 1 - 2 * core

    barrier = pltpu.get_barrier_semaphore()
    partners = [{"py": peer} for peer in peers.values()] + [{"px": twin}, {"px": other}]
    for partner in partners:
        pl.semaphore_signal(barrier, inc=1, device_id=partner, device_id_type=pl.DeviceIdType.MESH)

    loads = {}

    def load(name, src, dst):
        loads[name] = pltpu.make_async_copy(src, dst, sems_in.at[len(loads)])
        loads[name].start()

    load("first", dens_in.at[0], dens.at[0])
    load("fold_z", fold_z_in, fold_z)
    load("rest", dens_in.at[pl.ds(1, replicas - 1)], dens.at[pl.ds(1, replicas - 1)])
    load("factors", factors_in, factors)
    load("fold_y", fold_y_in, fold_y)
    load("wide", wide_in, wide)
    load("tall", tall_in, tall)
    load("back_tall", back_tall_in, back_tall)
    load("back_wide", back_wide_in, back_wide)
    load("open_y", open_y_in, open_y)
    load("open_z", open_z_in, open_z)

    def make(src, dst, sems, slot, device):
        return pltpu.make_async_remote_copy(
            src_ref=src, dst_ref=dst, send_sem=sems.at[(0,) + slot], recv_sem=sems.at[(1,) + slot],
            device_id=device, device_id_type=pl.DeviceIdType.MESH,
        )

    def span(chunk):
        return pl.ds(chunk * TILES, TILES)

    def lines(py):
        return pl.ds(pl.multiple_of(py * rows_y, 8), rows_y)

    def row(tile):
        return side * tile + (1 - side) * (rows_x - 1 - tile)

    def fold(replica, chunk):
        left = [dens[replica, row(chunk * TILES + i)] for i in range(TILES)]
        right = [dens[replica, row(tiles + chunk * TILES + i)] for i in range(TILES)]
        both = jnp.concatenate([jnp.concatenate(left, 0), jnp.concatenate(right, 0)], 1)
        waves = matmul(jnp.concatenate(halves(both), 1), fold_z[...])
        for parity in range(2):
            cut = waves[:, parity * length : (parity + 1) * length]
            a[replica, parity, span(chunk)] = cut.reshape(TILES, rows_y, length)

    sends_z = {}
    for chunk in range(chunks):
        for step, peer in peers.items():
            replica, parity = role(peer)
            sends_z[step, chunk] = make(
                a.at[replica, parity, span(chunk)], z.at[span(chunk), lines(me_py), :],
                sems_z, (step, chunk), {"py": peer},
            )
    def steps(replica):
        return ((3,), (2, 1)) if replica == 0 else ((2, 1), (3,))

    def scatter(replica, chunk):
        at_outer, at_inner = steps(replica)

        @pl.when(outer)
        def _():
            for step in at_outer:
                sends_z[step, chunk].start()

        @pl.when(jnp.logical_not(outer))
        def _():
            for step in at_inner:
                sends_z[step, chunk].start()

    loads["first"].wait()
    loads["fold_z"].wait()
    for replica in range(replicas):
        if replica == 1:
            loads["rest"].wait()
        for chunk in range(chunks):
            fold(replica, chunk)
            if replica == chunk == 0:
                pl.semaphore_wait(barrier, len(partners))
            scatter(replica, chunk)

    @pl.loop(0, tiles, unroll=4)
    def _(tile):
        z[tile, lines(me_py), :] = a[mine, odd_z, tile]

    def kernel_values():
        loads["factors"].wait()
        terms = factors.shape[1]
        flat[...] = jnp.zeros_like(flat)
        where = lax.broadcasted_iota(jnp.int32, (terms, length), 1)
        weight = jnp.where(where == 0, 0.5 / length, 1.0 / length)
        for dim in range(3):
            flat[dim, 0:terms] = factors[dim, :, 0:length] * weight
        for dim in range(2):
            turned[dim] = flat[dim].T
        high, low = halves(flat[2])
        gains[...] = jnp.concatenate(
            [jnp.concatenate([high, low], 1), jnp.concatenate([high, jnp.zeros_like(low)], 1)], 0
        )

        @pl.loop(0, length, unroll=8)
        def _(f):
            pair = turned[0] * turned[1, pl.ds(f, 1), :]
            sums = matmul(jnp.concatenate(halves(pair), 1), gains[...])
            kern[f] = sums[:, :length] + sums[:, length:]

    kernel_values()
    sends_y, sends_c = [], []

    def fold_lines(chunk):
        for step in peers:
            sends_z[step, chunk].wait_recv()
        for i in range(0, TILES, 2):
            tile = chunk * TILES + i
            cells = jnp.concatenate([z[tile], z[tile + 1]], 1)
            waves = matmul(fold_y[...], jnp.concatenate(halves(cells), 0))
            for parity in range(2):
                for j in range(2):
                    b[parity, tile + j] = waves[
                        parity * half : (parity + 1) * half, j * length : (j + 1) * length
                    ]
        copy = make(b.at[1 - side, span(chunk)], p.at[span(chunk)], sems_y, (chunk,), {"px": twin})
        copy.start()
        sends_y.append(copy)

    flip = sign.astype(jnp.float32)
    is_odd = core.astype(jnp.float32)
    even_or = (1.0 - is_odd) + is_odd * flip
    odd_or = (1.0 - is_odd) * flip + is_odd

    def fold_sheets(chunk):
        sends_y[chunk].wait_recv()
        for i in range(TILES):
            tile = chunk * TILES + i
            ours, theirs = b[side, tile], p[tile]
            total, gap = ours + theirs, (ours - theirs) * flip
            x[part, tile] = jnp.where(core == 0, total, gap)
            swap[tile] = jnp.where(core == 0, gap, total)
        copy = make(swap.at[span(chunk)], x.at[part, span(chunk)], sems_c, (chunk,), {"px": other})
        copy.start()
        sends_c.append(copy)

    def forward(chunk):
        sends_c[chunk].wait_recv()

        for where in range(2):
            cells = x[where, span(chunk)].reshape(TILES * half, length)
            high, low = halves(cells)
            waves = matmul(jnp.concatenate([high, low, high], 1), wide[odd_z])
            for i in range(TILES):
                high, low = halves(waves[i * half : (i + 1) * half])
                both = matmul(tall[side], jnp.concatenate([high, high, low], 0))
                for j in range(2):
                    start = (where * rows_x + j * tiles + chunk * TILES + i) * PITCH
                    e[pl.ds(pl.multiple_of(start, 8), length), :] = both[:, j * length : (j + 1) * length]

    for name in ("fold_y", "wide", "tall"):
        loads[name].wait()
    for stage in range(chunks + LAG + 1):
        if stage < chunks:
            fold_lines(stage)
        if 0 <= stage - LAG < chunks:
            fold_sheets(stage - LAG)
        if 0 <= stage - LAG - 1:
            forward(stage - LAG - 1)

    def middle():
        @pl.loop(0, length // 2, unroll=4)
        def _(f):
            cells = jnp.concatenate([e[pl.ds(2 * f + i, half, stride=PITCH), :] for i in range(2)], 1)
            high, low = halves(cells)
            waves = matmul(tall[core], jnp.concatenate([high, high, low], 0))
            product = waves * jnp.concatenate([kern[2 * f], kern[2 * f + 1]], 1)
            cells = matmul(back_tall[core], jnp.concatenate(halves(product), 0))
            cells = cells[:half] + cells[half:]
            for i in range(2):
                turned_e[pl.ds(2 * f + i, half, stride=PITCH), :] = cells[:, i * length : (i + 1) * length]

    loads["back_tall"].wait()
    middle()
    sends_ci, sends_yi, sends_zi = [], [], {}

    def backward(chunk):
        for where in (1 - part, part):
            found = []
            for i in range(TILES):
                cells = []
                for j in range(2):
                    start = (where * rows_x + j * tiles + chunk * TILES + i) * PITCH
                    cells.append(turned_e[pl.ds(pl.multiple_of(start, 8), length), :])
                cells = matmul(
                    back_tall[side], jnp.concatenate(halves(jnp.concatenate(cells, 1)), 0)
                )
                found.append(cells[:half] + cells[half:])
            high, low = halves(jnp.concatenate(found, 0))
            cells = matmul(jnp.concatenate([high, low, high], 1), back_wide[odd_z])
            cells = cells.reshape(TILES, half, length)
            if where is part:
                keep[span(chunk)] = cells
            else:
                c_send[span(chunk)] = cells
                copy = make(
                    c_send.at[span(chunk)], c_held.at[span(chunk)], sems_ci, (chunk,), {"px": other}
                )
                copy.start()
                sends_ci.append(copy)

    def open_sheets(chunk):
        sends_ci[chunk].wait_recv()
        for i in range(TILES):
            tile = chunk * TILES + i
            first, second = keep[tile], c_held[tile]
            even = jnp.where(core == 0, first, second)
            odd = jnp.where(core == 0, second, first) * flip
            g[side, tile] = even + odd
            g_send[tile] = even - odd
        copy = make(
            g_send.at[span(chunk)], g.at[side, span(chunk)], sems_yi, (chunk,), {"px": twin}
        )
        copy.start()
        sends_yi.append(copy)

    def open_lines(chunk):
        sends_yi[chunk].wait_recv()
        for i in range(0, TILES, 2):
            tile = chunk * TILES + i
            both = [
                jnp.concatenate([g[parity, tile], g[parity, tile + 1]], 1) for parity in range(2)
            ]
            cells = matmul(open_y[...], jnp.concatenate(halves(jnp.concatenate(both, 0)), 0))
            for j in range(2):
                zr[tile + j] = cells[:, j * length : (j + 1) * length]
        for step, peer in peers.items():
            sends_zi[step, chunk] = make(
                zr.at[span(chunk), lines(peer), :], fin.at[mine, odd_z, span(chunk)],
                sems_zi, (step, chunk), {"py": peer},
            )
        for step in (3, 2):
            sends_zi[step, chunk].start()

        @pl.when(jnp.logical_not(outer))
        def _():
            sends_zi[1, chunk].start()

        fin[mine, odd_z, span(chunk)] = zr[span(chunk), lines(me_py), :]

    for name in ("back_wide", "open_y", "open_z"):
        loads[name].wait()
    for stage in range(chunks + LAG + 1):
        if stage < chunks:
            backward(stage)
        if 0 <= stage - 1 < chunks:
            open_sheets(stage - 1)
        if 0 <= stage - LAG - 1:
            open_lines(stage - LAG - 1)

    @pl.when(outer)
    def _():
        for chunk in range(chunks):
            sends_zi[1, chunk].start()

    stores = []

    def finish(replica, chunk):
        at_outer, at_inner = steps(replica)

        @pl.when(outer)
        def _():
            for step in at_outer:
                sends_zi[step, chunk].wait_recv()

        @pl.when(jnp.logical_not(outer))
        def _():
            for step in at_inner:
                sends_zi[step, chunk].wait_recv()

        both = [
            fin[replica, parity, span(chunk)].reshape(TILES * rows_y, length) for parity in range(2)
        ]
        cells = matmul(
            jnp.concatenate(halves(jnp.concatenate(both, 1)), 1), open_z[...]
        )
        for i in range(TILES):
            cut = cells[i * rows_y : (i + 1) * rows_y]
            tile = chunk * TILES + i
            found[replica, row(tile)] = cut[:, :length]
            found[replica, row(tiles + tile)] = cut[:, length:]
        for part_x in range(2):
            first = part_x * tiles + chunk * TILES
            rows = pl.ds(side * first + (1 - side) * (rows_x - first - TILES), TILES)
            copy = pltpu.make_async_copy(
                found.at[replica, rows], out.at[replica, rows], sems_out.at[replica, chunk, part_x]
            )
            copy.start()
            stores.append(copy)

    for replica in range(replicas):
        for chunk in range(chunks):
            finish(replica, chunk)

    for copy in [*sends_z.values(), *sends_y, *sends_c, *sends_ci, *sends_yi, *sends_zi.values()]:
        copy.wait_send()
    for copy in stores:
        copy.wait()


def twice(table):
    zero = np.zeros_like(table)
    return np.block([[table, zero], [zero, table]])


def tables_of(length):
    half = length // 2
    angle = (np.arange(length)[:, None] * (2 * np.arange(half) + 1) % (4 * length)) * (math.pi / (2 * length))
    waves = np.stack([np.cos(angle), np.sin(angle)]).astype(np.float32)
    high = waves.astype(jnp.bfloat16).astype(np.float32)
    low = waves - high
    near, far = np.eye(half), np.eye(half)[::-1]
    line = np.block([[far, near], [-far, near]])
    sides = [line[:half].T, line[half:].T]
    fold_z = np.concatenate([twice(side) for side in sides], 1)
    fold_z = np.concatenate([fold_z, fold_z], 0)
    fold_y = np.concatenate([line, line], 1)
    open_y = np.concatenate([line.T, line.T], 1)
    open_z = np.concatenate([twice(side.T) for side in sides], 0)
    open_z = np.concatenate([open_z, open_z], 0)
    wide, tall, back_tall, back_wide = [], [], [], []
    for parity in range(2):
        up, down = high[parity], low[parity]
        wide.append(np.concatenate([twice(up.T), twice(up.T), twice(down.T)], 0))
        tall.append(np.concatenate([up, down, up], 1))
        back_tall.append(np.block([[up.T, up.T], [down.T, np.zeros_like(down.T)]]))
        back_wide.append(np.concatenate([twice(up), twice(up), twice(down)], 0))
    found = (fold_z, fold_y, np.stack(wide), np.stack(tall), np.stack(back_tall), np.stack(back_wide), open_y, open_z)
    return [jnp.asarray(table.astype(np.float32).astype(jnp.bfloat16)) for table in found]


def sector_body(density, kernel_factors):
    replicas, rows_x, rows_y, length = density.shape
    half, tiles = length // 2, rows_x // 2
    chunks = tiles // TILES
    count_px, count_py = lax.axis_size("px"), lax.axis_size("py")
    f32, bf16 = jnp.float32, jnp.bfloat16
    dma = pltpu.SemaphoreType.DMA
    sheet = (tiles, half, length)
    given = (density, kernel_factors, *tables_of(length))
    return pl.pallas_call(
        sector_kernel,
        out_shape=jax.ShapeDtypeStruct(density.shape, f32),
        in_specs=[pl.BlockSpec(memory_space=pl.ANY)] * len(given),
        out_specs=pl.BlockSpec(memory_space=pl.ANY),
        scratch_shapes=[pltpu.VMEM(array.shape, array.dtype) for array in given] + [
            pltpu.VMEM((replicas, 2, tiles, rows_y, length), f32),
            pltpu.VMEM((tiles, length, length), f32),
            pltpu.VMEM((2,) + sheet, f32), pltpu.VMEM(sheet, f32), pltpu.VMEM(sheet, f32),
            pltpu.VMEM((2,) + sheet, f32),
            pltpu.VMEM((half * PITCH, length), f32), pltpu.VMEM((half * PITCH, length), f32),
            pltpu.VMEM((length, length, length), f32),
            pltpu.VMEM(sheet, f32), pltpu.VMEM(sheet, f32), pltpu.VMEM(sheet, f32),
            pltpu.VMEM((2,) + sheet, f32), pltpu.VMEM(sheet, f32),
            pltpu.VMEM((tiles, length, length), f32),
            pltpu.VMEM((replicas, 2, tiles, rows_y, length), f32),
            pltpu.VMEM(density.shape, f32),
            pltpu.VMEM((3, length, length), f32), pltpu.VMEM((2, length, length), f32),
            pltpu.VMEM((2 * length, 2 * length), bf16),
            dma((2, count_py, chunks)), dma((2, chunks)), dma((2, chunks)),
            dma((2, chunks)), dma((2, chunks)), dma((2, count_py, chunks)),
            dma((len(given) + 1,)), dma((replicas, chunks, 2)),
        ],
        compiler_params=pltpu.CompilerParams(
            has_side_effects=True, vmem_limit_bytes=56 * 2**20, collective_id=0
        ),
    )(*given)


def body(density, kernel_factors):
    replicas, rows_x, rows_y, length = density.shape
    count_px, count_py = lax.axis_size("px"), lax.axis_size("py")
    square = count_px == count_py == 2 * replicas == 4
    whole = rows_x * count_px == rows_y * count_py == length == LANES
    if square and whole and kernel_factors.shape[1] <= LANES:
        return sector_body(density, kernel_factors)
    return plain_body(density, kernel_factors)


def solution(mesh):
    placed = (P("rep", "px", "py", None), P())
    return jax.shard_map(
        body, mesh=mesh, in_specs=placed, out_specs=P("rep", "px", "py", None), check_vma=False
    )
```

```python
import math

import jax
import jax.numpy as jnp
import numpy as np
from jax import lax
from jax.experimental import pallas as pl
from jax.experimental.pallas import tpu as pltpu
from jax.sharding import PartitionSpec as P

HIGHEST = lax.Precision.HIGHEST
LANES = 128
TILES = 2
LAG = 3
GROUP = 8
PITCH = 136


def spectral_table(length, chunks):
    freq = np.arange(length).reshape(chunks, 1, length // chunks, 1)
    angle = (freq * np.arange(length) % (2 * length)) * (math.pi / length)
    both = np.concatenate([np.cos(angle), np.sin(angle)], 1)
    return both.reshape(2 * length, length).astype(np.float32)


def dot(spec, left, right):
    return jnp.einsum(spec, left, right, precision=HIGHEST, preferred_element_type=jnp.float32)


def kernel_block(factors, y_start, y_count, z_start, z_count):
    length = factors.shape[2] // 2
    weights = np.full((length,), 1.0 / length, np.float32)
    weights[0] = 0.5 / length
    factors = factors[:, :, :length] * weights
    factor_y = lax.dynamic_slice_in_dim(factors[1], y_start, y_count, 1)
    factor_z = lax.dynamic_slice_in_dim(factors[2], z_start, z_count, 1)
    pair = factor_z[:, :, None] * factor_y[:, None, :]
    return jnp.einsum("gzy,gx->zyx", pair, factors[0], precision=lax.Precision.HIGHEST)


def plain_body(density, kernel_factors):
    replicas, rows_x, rows_y, length = density.shape
    count_px = lax.axis_size("px")
    count_py = lax.axis_size("py")
    half = count_px // replicas
    trade = [[i + half * r for r in range(replicas)] for i in range(half)]
    lines = [[r * half + i for i in range(half)] for r in range(replicas)]
    index_x = lax.axis_index("px") % half
    index_y = lax.axis_index("py")
    table_z = spectral_table(length, count_py)
    table_y = spectral_table(length, half)
    order = np.arange(length).reshape(replicas, half, rows_x).transpose(1, 0, 2).reshape(-1)
    table_x = spectral_table(length, 1)[:, order]

    held = lax.all_to_all(density, "px", 0, 0, axis_index_groups=trade, tiled=True)
    held = held.reshape(replicas * rows_x, rows_y, length)
    held = dot("kz,xyz->kyx", table_z, held)
    held = lax.all_to_all(held, "py", 0, 1, tiled=True)
    held = dot("qy,kyx->kqx", table_y, held)
    held = lax.all_to_all(held, "px", 1, 2, axis_index_groups=lines, tiled=True)
    z_freq, y_freq = length // count_py, length // half
    kernel = kernel_block(kernel_factors, index_x * y_freq, y_freq, index_y * z_freq, z_freq)
    held = dot("kqx,px->kqp", held, table_x)
    held = held.reshape(2, z_freq, 2, y_freq, 2, length) * kernel[None, :, None, :, None, :]
    held = held.reshape(2 * z_freq, 2 * y_freq, 2 * length)
    held = dot("kqp,px->kqx", held, table_x)
    held = lax.all_to_all(held, "px", 2, 1, axis_index_groups=lines, tiled=True)
    held = dot("kqx,qy->kyx", held, table_y)
    held = lax.all_to_all(held, "py", 1, 0, tiled=True)
    held = dot("kyx,kz->xyz", held, table_z)
    held = held.reshape(replicas, rows_x, rows_y, length)
    return lax.all_to_all(held, "px", 0, 0, axis_index_groups=trade, tiled=True)


def halves(values):
    high = values.astype(jnp.bfloat16)
    low = (values - high.astype(jnp.float32)).astype(jnp.bfloat16)
    return high, low


def matmul(left, right):
    return lax.dot_general(left, right, (((1,), (0,)), ((), ())), preferred_element_type=jnp.float32)


def sector_kernel(
    dens_in, factors_in, fold_z_in, fold_y_in, wide_in, tall_in, back_tall_in, back_wide_in, open_y_in, open_z_in, out,
    dens, factors, fold_z, fold_y, wide, tall, back_tall, back_wide, open_y, open_z,
    a, z, b, p, swap, x, e, turned_e, kern, keep, c_send, c_held, g, g_send, zr, fin,
    flat, turned, gains, solved,
    sems_z, sems_y, sems_c, sems_ci, sems_yi, sems_zi, sems_in,
):
    replicas, rows_x, rows_y, length = dens.shape
    half = length // 2
    tiles = rows_x // 2
    chunks = tiles // TILES
    me_px, me_py = lax.axis_index("px"), lax.axis_index("py")
    count_px, count_py = lax.axis_size("px"), lax.axis_size("py")
    side, core = lax.div(me_px, 2), lax.rem(me_px, 2)
    sign = 2 * side - 1
    part = side * (me_px - 2) + (1 - side) * (1 - me_px)
    peers = {1: me_py + 1 - 2 * lax.rem(me_py, 2), 2: lax.rem(me_py + 2, count_py), 3: count_py - 1 - me_py}

    def role(py):
        return lax.div(lax.rem(py + 1, count_py), 2), lax.div(py, 2)

    mine, odd_z = role(me_py)
    outer = mine == 0
    twin = count_px - 1 - me_px
    other = me_px + 1 - 2 * core

    barrier = pltpu.get_barrier_semaphore()
    partners = [{"py": peer} for peer in peers.values()] + [{"px": twin}, {"px": other}]
    for partner in partners:
        pl.semaphore_signal(barrier, inc=1, device_id=partner, device_id_type=pl.DeviceIdType.MESH)

    loads = {}

    def load(name, src, dst):
        loads[name] = pltpu.make_async_copy(src, dst, sems_in.at[len(loads)])
        loads[name].start()

    load("first", dens_in.at[0], dens.at[0])
    load("fold_z", fold_z_in, fold_z)
    load("rest", dens_in.at[pl.ds(1, replicas - 1)], dens.at[pl.ds(1, replicas - 1)])
    load("factors", factors_in, factors)
    load("fold_y", fold_y_in, fold_y)
    load("wide", wide_in, wide)
    load("tall", tall_in, tall)
    load("back_tall", back_tall_in, back_tall)
    load("back_wide", back_wide_in, back_wide)
    load("open_y", open_y_in, open_y)
    load("open_z", open_z_in, open_z)

    def make(src, dst, sems, slot, device):
        return pltpu.make_async_remote_copy(
            src_ref=src, dst_ref=dst, send_sem=sems.at[(0,) + slot], recv_sem=sems.at[(1,) + slot],
            device_id=device, device_id_type=pl.DeviceIdType.MESH,
        )

    def span(chunk):
        return pl.ds(chunk * TILES, TILES)

    def lines(py):
        return pl.ds(pl.multiple_of(py * rows_y, 8), rows_y)

    def row(tile):
        return side * tile + (1 - side) * (rows_x - 1 - tile)

    def fold(replica, chunk):
        left = [dens[replica, row(chunk * TILES + i)] for i in range(TILES)]
        right = [dens[replica, row(tiles + chunk * TILES + i)] for i in range(TILES)]
        both = jnp.concatenate([jnp.concatenate(left, 0), jnp.concatenate(right, 0)], 1)
        waves = matmul(jnp.concatenate(halves(both), 1), fold_z[...])
        for parity in range(2):
            cut = waves[:, parity * length : (parity + 1) * length]
            a[replica, parity, span(chunk)] = cut.reshape(TILES, rows_y, length)

    sends_z = {}
    for chunk in range(chunks):
        for step, peer in peers.items():
            replica, parity = role(peer)
            sends_z[step, chunk] = make(
                a.at[replica, parity, span(chunk)], z.at[span(chunk), lines(me_py), :],
                sems_z, (step, chunk), {"py": peer},
            )
    def steps(replica):
        return ((3,), (2, 1)) if replica == 0 else ((2, 1), (3,))

    def scatter(replica, chunk):
        at_outer, at_inner = steps(replica)

        @pl.when(outer)
        def _():
            for step in at_outer:
                sends_z[step, chunk].start()

        @pl.when(jnp.logical_not(outer))
        def _():
            for step in at_inner:
                sends_z[step, chunk].start()

    loads["first"].wait()
    loads["fold_z"].wait()
    for replica in range(replicas):
        if replica == 1:
            loads["rest"].wait()
        for chunk in range(chunks):
            fold(replica, chunk)
            if replica == chunk == 0:
                pl.semaphore_wait(barrier, len(partners))
            scatter(replica, chunk)

    @pl.loop(0, tiles, unroll=4)
    def _(tile):
        z[tile, lines(me_py), :] = a[mine, odd_z, tile]

    def kernel_values():
        loads["factors"].wait()
        terms = factors.shape[1]
        flat[...] = jnp.zeros_like(flat)
        where = lax.broadcasted_iota(jnp.int32, (terms, length), 1)
        weight = jnp.where(where == 0, 0.5 / length, 1.0 / length)
        for dim in range(3):
            flat[dim, 0:terms] = factors[dim, :, 0:length] * weight
        for dim in range(2):
            turned[dim] = flat[dim].T
        high, low = halves(flat[2])
        gains[...] = jnp.concatenate(
            [jnp.concatenate([high, low], 1), jnp.concatenate([high, jnp.zeros_like(low)], 1)], 0
        )

        @pl.loop(0, length, unroll=8)
        def _(f):
            pair = turned[0] * turned[1, pl.ds(f, 1), :]
            sums = matmul(jnp.concatenate(halves(pair), 1), gains[...])
            kern[f] = sums[:, :length] + sums[:, length:]

    kernel_values()
    sends_y, sends_c = [], []

    def fold_lines(chunk):
        for step in peers:
            sends_z[step, chunk].wait_recv()
        for i in range(0, TILES, 2):
            tile = chunk * TILES + i
            cells = jnp.concatenate([z[tile], z[tile + 1]], 1)
            waves = matmul(fold_y[...], jnp.concatenate(halves(cells), 0))
            for parity in range(2):
                for j in range(2):
                    b[parity, tile + j] = waves[
                        parity * half : (parity + 1) * half, j * length : (j + 1) * length
                    ]
        copy = make(b.at[1 - side, span(chunk)], p.at[span(chunk)], sems_y, (chunk,), {"px": twin})
        copy.start()
        sends_y.append(copy)

    flip = sign.astype(jnp.float32)
    is_odd = core.astype(jnp.float32)
    even_or = (1.0 - is_odd) + is_odd * flip
    odd_or = (1.0 - is_odd) * flip + is_odd

    def fold_sheets(chunk):
        sends_y[chunk].wait_recv()
        for i in range(TILES):
            tile = chunk * TILES + i
            ours, theirs = b[side, tile], p[tile]
            total, gap = ours + theirs, (ours - theirs) * flip
            x[part, tile] = jnp.where(core == 0, total, gap)
            swap[tile] = jnp.where(core == 0, gap, total)
        copy = make(swap.at[span(chunk)], x.at[part, span(chunk)], sems_c, (chunk,), {"px": other})
        copy.start()
        sends_c.append(copy)

    def forward(chunk):
        sends_c[chunk].wait_recv()

        for where in range(2):
            cells = x[where, span(chunk)].reshape(TILES * half, length)
            high, low = halves(cells)
            waves = matmul(jnp.concatenate([high, low, high], 1), wide[odd_z])
            for i in range(TILES):
                high, low = halves(waves[i * half : (i + 1) * half])
                both = matmul(tall[side], jnp.concatenate([high, high, low], 0))
                for j in range(2):
                    start = (where * rows_x + j * tiles + chunk * TILES + i) * PITCH
                    e[pl.ds(pl.multiple_of(start, 8), length), :] = both[:, j * length : (j + 1) * length]

    for name in ("fold_y", "wide", "tall"):
        loads[name].wait()
    for stage in range(chunks + LAG + 1):
        if stage < chunks:
            fold_lines(stage)
        if 0 <= stage - LAG < chunks:
            fold_sheets(stage - LAG)
        if 0 <= stage - LAG - 1:
            forward(stage - LAG - 1)

    def spectra(f):
        for k in range(GROUP):
            first = 2 * (f * GROUP + k)
            cells = jnp.concatenate([e[pl.ds(first + i, half, stride=PITCH), :] for i in range(2)], 1)
            high, low = halves(cells)
            waves = matmul(tall[core], jnp.concatenate([high, high, low], 0))
            product = waves * jnp.concatenate([kern[first], kern[first + 1]], 1)
            solved[k] = jnp.concatenate(halves(product), 0)

    def answers(f):
        for k in range(GROUP):
            first = 2 * (f * GROUP + k)
            cells = matmul(back_tall[core], solved[k])
            cells = cells[:half] + cells[half:]
            for i in range(2):
                turned_e[pl.ds(first + i, half, stride=PITCH), :] = cells[:, i * length : (i + 1) * length]

    def middle():
        trips = length // (2 * GROUP)
        spectra(0)

        @pl.loop(1, trips)
        def _(f):
            answers(f - 1)
            spectra(f)

        answers(trips - 1)

    loads["back_tall"].wait()
    middle()
    sends_ci, sends_yi, sends_zi = [], [], {}

    def backward(chunk):
        solved_here = []
        for where in (1 - part, part):
            rows = []
            for i in range(TILES):
                cells = []
                for j in range(2):
                    start = (where * rows_x + j * tiles + chunk * TILES + i) * PITCH
                    cells.append(turned_e[pl.ds(pl.multiple_of(start, 8), length), :])
                cells = matmul(
                    back_tall[side], jnp.concatenate(halves(jnp.concatenate(cells, 1)), 0)
                )
                rows.append(cells[:half] + cells[half:])
            high, low = halves(jnp.concatenate(rows, 0))
            cells = matmul(jnp.concatenate([high, low, high], 1), back_wide[odd_z])
            solved_here.append(cells.reshape(TILES, half, length))
        c_send[span(chunk)], keep[span(chunk)] = solved_here
        copy = make(c_send.at[span(chunk)], c_held.at[span(chunk)], sems_ci, (chunk,), {"px": other})
        copy.start()
        sends_ci.append(copy)

    def open_sheets(chunk):
        sends_ci[chunk].wait_recv()
        for i in range(TILES):
            tile = chunk * TILES + i
            first, second = keep[tile], c_held[tile]
            even = jnp.where(core == 0, first, second)
            odd = jnp.where(core == 0, second, first) * flip
            g[side, tile] = even + odd
            g_send[tile] = even - odd
        copy = make(
            g_send.at[span(chunk)], g.at[side, span(chunk)], sems_yi, (chunk,), {"px": twin}
        )
        copy.start()
        sends_yi.append(copy)

    def open_lines(chunk):
        sends_yi[chunk].wait_recv()
        for i in range(0, TILES, 2):
            tile = chunk * TILES + i
            both = [
                jnp.concatenate([g[parity, tile], g[parity, tile + 1]], 1) for parity in range(2)
            ]
            cells = matmul(open_y[...], jnp.concatenate(halves(jnp.concatenate(both, 0)), 0))
            for j in range(2):
                zr[tile + j] = cells[:, j * length : (j + 1) * length]
        for step, peer in peers.items():
            sends_zi[step, chunk] = make(
                zr.at[span(chunk), lines(peer), :], fin.at[mine, odd_z, span(chunk)],
                sems_zi, (step, chunk), {"py": peer},
            )
        for step in (3, 2):
            sends_zi[step, chunk].start()

        @pl.when(jnp.logical_not(outer))
        def _():
            sends_zi[1, chunk].start()

        fin[mine, odd_z, span(chunk)] = zr[span(chunk), lines(me_py), :]

    for name in ("back_wide", "open_y", "open_z"):
        loads[name].wait()
    for stage in range(chunks + LAG + 1):
        if stage < chunks:
            backward(stage)
        if 0 <= stage - 1 < chunks:
            open_sheets(stage - 1)
        if 0 <= stage - LAG - 1:
            open_lines(stage - LAG - 1)

    @pl.when(outer)
    def _():
        for chunk in range(chunks):
            sends_zi[1, chunk].start()

    for copy in [*sends_z.values(), *sends_y, *sends_c, *sends_ci, *sends_yi]:
        copy.wait_send()

    def finish(replica, chunk):
        at_outer, at_inner = steps(replica)

        @pl.when(outer)
        def _():
            for step in at_outer:
                sends_zi[step, chunk].wait_recv()

        @pl.when(jnp.logical_not(outer))
        def _():
            for step in at_inner:
                sends_zi[step, chunk].wait_recv()

        both = [
            fin[replica, parity, span(chunk)].reshape(TILES * rows_y, length) for parity in range(2)
        ]
        cells = matmul(
            jnp.concatenate(halves(jnp.concatenate(both, 1)), 1), open_z[...]
        )
        for i in range(TILES):
            cut = cells[i * rows_y : (i + 1) * rows_y]
            tile = chunk * TILES + i
            out[replica, row(tile)] = cut[:, :length]
            out[replica, row(tiles + tile)] = cut[:, length:]

    for replica in range(replicas):
        for chunk in range(chunks):
            if replica == 1 and chunk == chunks - 1:
                for copy in sends_zi.values():
                    copy.wait_send()
            finish(replica, chunk)


def twice(table):
    zero = np.zeros_like(table)
    return np.block([[table, zero], [zero, table]])


def tables_of(length):
    half = length // 2
    angle = (np.arange(length)[:, None] * (2 * np.arange(half) + 1) % (4 * length)) * (math.pi / (2 * length))
    waves = np.stack([np.cos(angle), np.sin(angle)]).astype(np.float32)
    high = waves.astype(jnp.bfloat16).astype(np.float32)
    low = waves - high
    near, far = np.eye(half), np.eye(half)[::-1]
    line = np.block([[far, near], [-far, near]])
    sides = [line[:half].T, line[half:].T]
    fold_z = np.concatenate([twice(side) for side in sides], 1)
    fold_z = np.concatenate([fold_z, fold_z], 0)
    fold_y = np.concatenate([line, line], 1)
    open_y = np.concatenate([line.T, line.T], 1)
    open_z = np.concatenate([twice(side.T) for side in sides], 0)
    open_z = np.concatenate([open_z, open_z], 0)
    wide, tall, back_tall, back_wide = [], [], [], []
    for parity in range(2):
        up, down = high[parity], low[parity]
        wide.append(np.concatenate([twice(up.T), twice(up.T), twice(down.T)], 0))
        tall.append(np.concatenate([up, down, up], 1))
        back_tall.append(np.block([[up.T, up.T], [down.T, np.zeros_like(down.T)]]))
        back_wide.append(np.concatenate([twice(up), twice(up), twice(down)], 0))
    found = (fold_z, fold_y, np.stack(wide), np.stack(tall), np.stack(back_tall), np.stack(back_wide), open_y, open_z)
    return [jnp.asarray(table.astype(np.float32).astype(jnp.bfloat16)) for table in found]


def sector_body(density, kernel_factors):
    replicas, rows_x, rows_y, length = density.shape
    half, tiles = length // 2, rows_x // 2
    chunks = tiles // TILES
    count_px, count_py = lax.axis_size("px"), lax.axis_size("py")
    f32, bf16 = jnp.float32, jnp.bfloat16
    dma = pltpu.SemaphoreType.DMA
    sheet = (tiles, half, length)
    given = [
        pltpu.with_memory_space_constraint(array, pltpu.HBM)
        for array in (density, kernel_factors, *tables_of(length))
    ]
    return pl.pallas_call(
        sector_kernel,
        out_shape=pltpu.VMEM(density.shape, f32),
        in_specs=[pl.BlockSpec(memory_space=pl.ANY)] * len(given),
        out_specs=pl.BlockSpec(memory_space=pltpu.VMEM),
        scratch_shapes=[pltpu.VMEM(array.shape, array.dtype) for array in given] + [
            pltpu.VMEM((replicas, 2, tiles, rows_y, length), f32),
            pltpu.VMEM((tiles, length, length), f32),
            pltpu.VMEM((2,) + sheet, f32), pltpu.VMEM(sheet, f32), pltpu.VMEM(sheet, f32),
            pltpu.VMEM((2,) + sheet, f32),
            pltpu.VMEM((half * PITCH, length), f32), pltpu.VMEM((half * PITCH, length), f32),
            pltpu.VMEM((length, length, length), f32),
            pltpu.VMEM(sheet, f32), pltpu.VMEM(sheet, f32), pltpu.VMEM(sheet, f32),
            pltpu.VMEM((2,) + sheet, f32), pltpu.VMEM(sheet, f32),
            pltpu.VMEM((tiles, length, length), f32),
            pltpu.VMEM((replicas, 2, tiles, rows_y, length), f32),
            pltpu.VMEM((3, length, length), f32), pltpu.VMEM((2, length, length), f32),
            pltpu.VMEM((2 * length, 2 * length), bf16),
            pltpu.VMEM((GROUP, 2 * length, 2 * length), bf16),
            dma((2, count_py, chunks)), dma((2, chunks)), dma((2, chunks)),
            dma((2, chunks)), dma((2, chunks)), dma((2, count_py, chunks)),
            dma((len(given) + 1,)),
        ],
        compiler_params=pltpu.CompilerParams(
            has_side_effects=True, vmem_limit_bytes=56 * 2**20, collective_id=0
        ),
    )(*given)


def body(density, kernel_factors):
    replicas, rows_x, rows_y, length = density.shape
    count_px, count_py = lax.axis_size("px"), lax.axis_size("py")
    square = count_px == count_py == 2 * replicas == 4
    whole = rows_x * count_px == rows_y * count_py == length == LANES
    if square and whole and kernel_factors.shape[1] <= LANES:
        return sector_body(density, kernel_factors)
    return plain_body(density, kernel_factors)


def solution(mesh):
    placed = (P("rep", "px", "py", None), P())
    return jax.shard_map(
        body, mesh=mesh, in_specs=placed, out_specs=P("rep", "px", "py", None), check_vma=False
    )
```

```python
import math

import jax
import jax.numpy as jnp
import numpy as np
from jax import lax
from jax.experimental import pallas as pl
from jax.experimental.pallas import tpu as pltpu
from jax.sharding import PartitionSpec as P

HIGHEST = lax.Precision.HIGHEST
LANES = 128
TILES = 2
LAG = 3
LAG_BACK = 3
GROUP = 8
PITCH = 129


def spectral_table(length, chunks):
    freq = np.arange(length).reshape(chunks, 1, length // chunks, 1)
    angle = (freq * np.arange(length) % (2 * length)) * (math.pi / length)
    both = np.concatenate([np.cos(angle), np.sin(angle)], 1)
    return both.reshape(2 * length, length).astype(np.float32)


def dot(spec, left, right):
    return jnp.einsum(spec, left, right, precision=HIGHEST, preferred_element_type=jnp.float32)


def kernel_block(factors, y_start, y_count, z_start, z_count):
    length = factors.shape[2] // 2
    weights = np.full((length,), 1.0 / length, np.float32)
    weights[0] = 0.5 / length
    factors = factors[:, :, :length] * weights
    factor_y = lax.dynamic_slice_in_dim(factors[1], y_start, y_count, 1)
    factor_z = lax.dynamic_slice_in_dim(factors[2], z_start, z_count, 1)
    pair = factor_z[:, :, None] * factor_y[:, None, :]
    return jnp.einsum("gzy,gx->zyx", pair, factors[0], precision=lax.Precision.HIGHEST)


def plain_body(density, kernel_factors):
    replicas, rows_x, rows_y, length = density.shape
    count_px = lax.axis_size("px")
    count_py = lax.axis_size("py")
    half = count_px // replicas
    trade = [[i + half * r for r in range(replicas)] for i in range(half)]
    lines = [[r * half + i for i in range(half)] for r in range(replicas)]
    index_x = lax.axis_index("px") % half
    index_y = lax.axis_index("py")
    table_z = spectral_table(length, count_py)
    table_y = spectral_table(length, half)
    order = np.arange(length).reshape(replicas, half, rows_x).transpose(1, 0, 2).reshape(-1)
    table_x = spectral_table(length, 1)[:, order]

    held = lax.all_to_all(density, "px", 0, 0, axis_index_groups=trade, tiled=True)
    held = held.reshape(replicas * rows_x, rows_y, length)
    held = dot("kz,xyz->kyx", table_z, held)
    held = lax.all_to_all(held, "py", 0, 1, tiled=True)
    held = dot("qy,kyx->kqx", table_y, held)
    held = lax.all_to_all(held, "px", 1, 2, axis_index_groups=lines, tiled=True)
    z_freq, y_freq = length // count_py, length // half
    kernel = kernel_block(kernel_factors, index_x * y_freq, y_freq, index_y * z_freq, z_freq)
    held = dot("kqx,px->kqp", held, table_x)
    held = held.reshape(2, z_freq, 2, y_freq, 2, length) * kernel[None, :, None, :, None, :]
    held = held.reshape(2 * z_freq, 2 * y_freq, 2 * length)
    held = dot("kqp,px->kqx", held, table_x)
    held = lax.all_to_all(held, "px", 2, 1, axis_index_groups=lines, tiled=True)
    held = dot("kqx,qy->kyx", held, table_y)
    held = lax.all_to_all(held, "py", 1, 0, tiled=True)
    held = dot("kyx,kz->xyz", held, table_z)
    held = held.reshape(replicas, rows_x, rows_y, length)
    return lax.all_to_all(held, "px", 0, 0, axis_index_groups=trade, tiled=True)


def halves(values):
    high = values.astype(jnp.bfloat16)
    low = (values - high.astype(jnp.float32)).astype(jnp.bfloat16)
    return high, low


def matmul(left, right):
    return lax.dot_general(left, right, (((1,), (0,)), ((), ())), preferred_element_type=jnp.float32)


def sector_kernel(
    dens_in, factors_in, tables_in, out,
    dens, factors, tables,
    a, z, b, p, swap, x, e, turned_e, kern, keep, c_send, c_held, g, g_send, zr, fin,
    flat, turned, gains, solved,
    sent, sems_z, sems_y, sems_c, sems_ci, sems_yi, sems_zi, sems_in,
):
    replicas, rows_x, rows_y, length = dens.shape
    half = length // 2
    tiles = rows_x // 2
    sizes = [TILES] * (tiles // TILES - 1) + [1] * TILES
    coming = [pl.ds(sum(sizes[:i]), size) for i, size in enumerate(sizes)]
    sizes = sizes[::-1]
    going = [pl.ds(sum(sizes[:i]), size) for i, size in enumerate(sizes)]
    chunks = len(sizes)
    me_px, me_py = lax.axis_index("px"), lax.axis_index("py")
    count_px, count_py = lax.axis_size("px"), lax.axis_size("py")
    side, core = lax.div(me_px, 2), lax.rem(me_px, 2)
    sign = 2 * side - 1
    part = side * (me_px - 2) + (1 - side) * (1 - me_px)
    peers = {1: me_py + 1 - 2 * lax.rem(me_py, 2), 2: lax.rem(me_py + 2, count_py), 3: count_py - 1 - me_py}

    def role(py):
        return lax.div(lax.rem(py + 1, count_py), 2), lax.div(py, 2)

    mine, odd_z = role(me_py)
    outer = mine == 0
    twin = count_px - 1 - me_px
    other = me_px + 1 - 2 * core

    barrier = pltpu.get_barrier_semaphore()
    partners = [{"py": peer} for peer in peers.values()] + [{"px": twin}, {"px": other}]
    for partner in partners:
        pl.semaphore_signal(barrier, inc=1, device_id=partner, device_id_type=pl.DeviceIdType.MESH)

    where_of, _ = layout_of(length)

    def table(name, parity=None):
        start, rows = where_of[name]
        if parity is None:
            return tables[start : start + rows, :]
        rows //= 2
        return tables[pl.ds(pl.multiple_of(start + parity * rows, 16), rows), :]

    loads = {}

    def load(name, src, dst):
        loads[name] = pltpu.make_async_copy(src, dst, sems_in.at[len(loads)])
        loads[name].start()

    early = pl.ds(0, where_of["fold_z"][1])
    late = pl.ds(early.size, tables.shape[0] - early.size)
    load("first", dens_in.at[0], dens.at[0])
    load("fold_z", tables_in.at[early], tables.at[early])
    load("rest", dens_in.at[pl.ds(1, replicas - 1)], dens.at[pl.ds(1, replicas - 1)])
    load("factors", factors_in, factors)
    load("tables", tables_in.at[late], tables.at[late])

    def make(src, dst, stage, sem, device):
        return pltpu.make_async_remote_copy(
            src_ref=src, dst_ref=dst, send_sem=sent.at[stage], recv_sem=sem,
            device_id=device, device_id_type=pl.DeviceIdType.MESH,
        )

    def arrived(ref, sem):
        make(ref, ref, 0, sem, {"px": other}).wait_recv()

    def gone(ref, stage):
        make(ref, ref, stage, sems_y.at[0], {"px": other}).wait_send()

    def lines(py):
        return pl.ds(pl.multiple_of(py * rows_y, 8), rows_y)

    three = pl.ds(0, (count_py - 1) * rows_y)

    def row(tile):
        return side * tile + (1 - side) * (rows_x - 1 - tile)

    def fold(replica, chunk):
        span = coming[chunk]
        left = [dens[replica, row(span.start + i)] for i in range(span.size)]
        right = [dens[replica, row(tiles + span.start + i)] for i in range(span.size)]
        both = jnp.concatenate([jnp.concatenate(left, 0), jnp.concatenate(right, 0)], 1)
        waves = matmul(jnp.concatenate(halves(both), 1), table("fold_z"))
        for parity in range(2):
            cut = waves[:, parity * length : (parity + 1) * length]
            a[replica, parity, span] = cut.reshape(span.size, rows_y, length)

    sends_z = {}
    for chunk in range(chunks):
        for step, peer in peers.items():
            replica, parity = role(peer)
            sends_z[step, chunk] = make(
                a.at[replica, parity, coming[chunk]], z.at[coming[chunk], lines(me_py), :],
                0, sems_z.at[chunk], {"py": peer},
            )

    def steps(replica):
        return ((3,), (2, 1)) if replica == 0 else ((2, 1), (3,))

    def scatter(replica, chunk):
        at_outer, at_inner = steps(replica)

        @pl.when(outer)
        def _():
            for step in at_outer:
                sends_z[step, chunk].start()

        @pl.when(jnp.logical_not(outer))
        def _():
            for step in at_inner:
                sends_z[step, chunk].start()

    loads["first"].wait()
    loads["fold_z"].wait()
    for replica in range(replicas):
        if replica == 1:
            loads["rest"].wait()
        for chunk in range(chunks):
            fold(replica, chunk)
            if replica == chunk == 0:
                pl.semaphore_wait(barrier, len(partners))
            scatter(replica, chunk)

    @pl.loop(0, tiles, unroll=4)
    def _(tile):
        z[tile, lines(me_py), :] = a[mine, odd_z, tile]

    def kernel_values():
        loads["factors"].wait()
        terms = factors.shape[1]
        flat[...] = jnp.zeros_like(flat)
        where = lax.broadcasted_iota(jnp.int32, (terms, length), 1)
        weight = jnp.where(where == 0, 0.5 / length, 1.0 / length)
        for dim in range(3):
            flat[dim, 0:terms] = factors[dim, :, 0:length] * weight
        for dim in range(2):
            turned[dim] = flat[dim].T
        high, low = halves(flat[2])
        gains[...] = jnp.concatenate(
            [jnp.concatenate([high, low], 1), jnp.concatenate([high, jnp.zeros_like(low)], 1)], 0
        )

        @pl.loop(0, length, unroll=8)
        def _(f):
            pair = turned[0] * turned[1, pl.ds(f, 1), :]
            sums = matmul(jnp.concatenate(halves(pair), 1), gains[...])
            kern[f] = sums[:, :length] + sums[:, length:]

    kernel_values()
    def fold_lines(chunk):
        span = coming[chunk]
        arrived(z.at[span, three, :], sems_z.at[chunk])
        for tile in range(span.start, span.start + span.size, 2):
            width = min(2, span.start + span.size - tile)
            cells = jnp.concatenate([z[tile + j] for j in range(width)], 1)
            waves = matmul(table("fold_y"), jnp.concatenate(halves(cells), 0))
            for parity in range(2):
                for j in range(width):
                    b[parity, tile + j] = waves[
                        parity * half : (parity + 1) * half, j * length : (j + 1) * length
                    ]
        make(b.at[1 - side, span], p.at[span], 1, sems_y.at[chunk], {"px": twin}).start()

    flip = sign.astype(jnp.float32)
    def fold_sheets(chunk):
        span = coming[chunk]
        arrived(p.at[span], sems_y.at[chunk])
        for tile in range(span.start, span.start + span.size):
            ours, theirs = b[side, tile], p[tile]
            total, gap = ours + theirs, (ours - theirs) * flip
            x[part, tile] = jnp.where(core == 0, total, gap)
            swap[tile] = jnp.where(core == 0, gap, total)
        make(swap.at[span], x.at[part, span], 2, sems_c.at[chunk], {"px": other}).start()

    def forward(start, count, wheres):
        cells = [x[where, pl.ds(start, count)].reshape(count * half, length) for where in wheres]
        high, low = halves(jnp.concatenate(cells, 0))
        waves = matmul(jnp.concatenate([high, low, high], 1), table("wide", odd_z))
        tall = table("tall", side)[:, : 3 * half]
        found = []
        for i in range(count * len(wheres)):
            high, low = halves(waves[i * half : (i + 1) * half])
            found.append(matmul(tall, jnp.concatenate([high, high, low], 0)))
        for k, where in enumerate(wheres):
            for i in range(count):
                for j in range(2):
                    first = (where * rows_x + j * tiles + start + i) * PITCH
                    e[pl.ds(first, length), :] = found[k * count + i][
                        :, j * length : (j + 1) * length
                    ]

    def forward_both(chunk, count):
        for one in range(chunk, chunk + count):
            arrived(swap.at[coming[one]], sems_c.at[one])
        tiles_here = sum(span.size for span in coming[chunk : chunk + count])
        forward(coming[chunk].start, tiles_here, (part, 1 - part))

    def forward_last():
        arrived(swap.at[coming[-1]], sems_c.at[chunks - 1])
        forward(coming[-1].start, coming[-1].size, (1 - part,))

    loads["tables"].wait()
    for stage in range(chunks + LAG + 1):
        if stage < chunks:
            fold_lines(stage)
        if 0 <= stage - LAG < chunks:
            fold_sheets(stage - LAG)
        if stage - LAG == chunks - 1:
            forward(coming[-1].start, coming[-1].size, (part,))
        ready = stage - LAG - 3
        if ready >= 0 and ready % 2 == 0:
            forward_both(ready, 2)
    forward_last()

    def spectrum(first):
        cells = jnp.concatenate([e[pl.ds(first + i, half, stride=PITCH), :] for i in range(2)], 1)
        high, low = halves(cells)
        return matmul(table("tall", core)[:, : 3 * half], jnp.concatenate([high, high, low], 0))

    def answer_of(first, k):
        cells = matmul(table("back_tall", core), solved[k])
        cells = cells[:half] + cells[half:]
        for i in range(2):
            turned_e[pl.ds(first + i, half, stride=PITCH), :] = cells[:, i * length : (i + 1) * length]

    def solve(first, k, waves):
        product = waves * jnp.concatenate([kern[first], kern[first + 1]], 1)
        solved[k] = jnp.concatenate(halves(product), 0)

    def middle():
        trips = length // (2 * GROUP)
        for k in range(GROUP):
            solve(2 * k, k, spectrum(2 * k))

        @pl.loop(1, trips)
        def _(f):
            for k in range(GROUP):
                first = 2 * (f * GROUP + k)
                waves = spectrum(first)
                answer_of(first - 2 * GROUP, k)
                solve(first, k, waves)

        for k in range(GROUP):
            answer_of(length - 2 * GROUP + 2 * k, k)

    middle()

    def backward(chunk):
        span = going[chunk]
        rows = []
        for where in (1 - part, part):
            for i in range(span.size):
                cells = []
                for j in range(2):
                    start = (where * rows_x + j * tiles + span.start + i) * PITCH
                    cells.append(turned_e[pl.ds(start, length), :])
                cells = jnp.concatenate(halves(jnp.concatenate(cells, 1)), 0)
                cells = matmul(table("back_tall", side), cells)
                rows.append(cells[:half] + cells[half:])
        high, low = halves(jnp.concatenate(rows, 0))
        wide = table("back_wide", odd_z)
        wide = jnp.concatenate([wide[:, :length], wide[:, length:]], 0)
        cells = matmul(jnp.concatenate([high, low, high], 1), wide)
        found = cells.reshape(2, span.size, half, length)
        c_send[span], keep[span] = found[0], found[1]
        make(c_send.at[span], c_held.at[span], 3, sems_ci.at[chunk], {"px": other}).start()

    def open_sheets(chunk):
        span = going[chunk]
        arrived(c_held.at[span], sems_ci.at[chunk])
        for tile in range(span.start, span.start + span.size):
            first, second = keep[tile], c_held[tile]
            even = jnp.where(core == 0, first, second)
            odd = jnp.where(core == 0, second, first) * flip
            g[side, tile] = even + odd
            g_send[tile] = even - odd
        make(g_send.at[span], g.at[side, span], 4, sems_yi.at[chunk], {"px": twin}).start()

    def answer(step, chunk):
        span = going[chunk]
        return make(
            zr.at[span, lines(peers[step]), :], fin.at[mine, odd_z, span],
            5, sems_zi.at[mine, chunk], {"py": peers[step]},
        )

    def open_lines(chunk):
        span = going[chunk]
        arrived(g_send.at[span], sems_yi.at[chunk])
        for tile in range(span.start, span.start + span.size, 2):
            width = min(2, span.start + span.size - tile)
            both = [
                jnp.concatenate([g[parity, tile + j] for j in range(width)], 1) for parity in range(2)
            ]
            cells = matmul(table("open_y"), jnp.concatenate(halves(jnp.concatenate(both, 0)), 0))
            for j in range(width):
                zr[tile + j] = cells[:, j * length : (j + 1) * length]
        for step in (3, 2):
            answer(step, chunk).start()

        @pl.when(jnp.logical_not(outer))
        def _():
            answer(1, chunk).start()

        fin[mine, odd_z, span] = zr[span, lines(me_py), :]

    for stage in range(chunks + LAG_BACK + 1):
        if stage < chunks:
            backward(stage)
        if 0 <= stage - 1 < chunks:
            open_sheets(stage - 1)
        if 0 <= stage - LAG_BACK - 1:
            open_lines(stage - LAG_BACK - 1)

    @pl.when(outer)
    def _():
        for chunk in range(chunks):
            answer(1, chunk).start()

    for stage, ref in enumerate((z.at[:, three, :], p, swap, c_send, g_send)):
        gone(ref, stage)

    def finish(replica, chunk):
        span = going[chunk]
        few, many = (outer, jnp.logical_not(outer))[:: 1 - 2 * replica]

        @pl.when(few)
        def _():
            arrived(fin.at[replica, 0, span], sems_zi.at[replica, chunk])

        @pl.when(many)
        def _():
            arrived(fin.at[replica, :, span], sems_zi.at[replica, chunk])

        both = [fin[replica, parity, span].reshape(span.size * rows_y, length) for parity in range(2)]
        cells = matmul(jnp.concatenate(halves(jnp.concatenate(both, 1)), 1), table("open_z"))
        for i in range(span.size):
            cut = cells[i * rows_y : (i + 1) * rows_y]
            out[replica, row(span.start + i)] = cut[:, :length]
            out[replica, row(tiles + span.start + i)] = cut[:, length:]

    for replica in range(replicas):
        for chunk in range(chunks):
            if replica == 1 and chunk == chunks - 1:
                gone(zr.at[:, three, :], 5)
            finish(replica, chunk)


def twice(table):
    zero = np.zeros_like(table)
    return np.block([[table, zero], [zero, table]])


def tables_of(length):
    half = length // 2
    angle = (np.arange(length)[:, None] * (2 * np.arange(half) + 1) % (4 * length)) * (math.pi / (2 * length))
    waves = np.stack([np.cos(angle), np.sin(angle)]).astype(np.float32)
    high = waves.astype(jnp.bfloat16).astype(np.float32)
    low = waves - high
    near, far = np.eye(half), np.eye(half)[::-1]
    line = np.block([[far, near], [-far, near]])
    sides = [line[:half].T, line[half:].T]
    fold_z = np.concatenate([twice(side) for side in sides], 1)
    fold_z = np.concatenate([fold_z, fold_z], 0)
    fold_y = np.concatenate([line, line], 1)
    open_y = np.concatenate([line.T, line.T], 1)
    open_z = np.concatenate([twice(side.T) for side in sides], 0)
    open_z = np.concatenate([open_z, open_z], 0)
    wide, tall, back_tall, back_wide = [], [], [], []
    for parity in range(2):
        up, down = high[parity], low[parity]
        wide.append(np.concatenate([twice(up.T), twice(up.T), twice(down.T)], 0))
        tall.append(np.concatenate([up, down, up], 1))
        back_tall.append(np.block([[up.T, up.T], [down.T, np.zeros_like(down.T)]]))
        back_wide.append(np.concatenate([twice(up), twice(up), twice(down)], 0))
    tall = np.concatenate(tall, 0)
    back_wide = [np.concatenate(np.split(one, 2, 0), 1) for one in back_wide]
    found = {
        "fold_z": fold_z, "fold_y": fold_y, "wide": np.concatenate(wide, 0),
        "tall": np.pad(tall, ((0, 0), (0, 2 * length - tall.shape[1]))),
        "back_tall": np.concatenate(back_tall, 0), "back_wide": np.concatenate(back_wide, 0),
        "open_y": open_y, "open_z": open_z,
    }
    return {name: one.astype(np.float32).astype(jnp.bfloat16) for name, one in found.items()}


def layout_of(length):
    found, start = {}, 0
    tables = tables_of(length)
    for name, one in tables.items():
        found[name] = (start, one.shape[0])
        start += one.shape[0]
    return found, np.concatenate(list(tables.values()), 0)


def sector_body(density, kernel_factors):
    replicas, rows_x, rows_y, length = density.shape
    half, tiles = length // 2, rows_x // 2
    chunks = tiles // TILES - 1 + TILES
    f32, bf16 = jnp.float32, jnp.bfloat16
    dma = pltpu.SemaphoreType.DMA
    sheet = (tiles, half, length)
    given = [
        pltpu.with_memory_space_constraint(array, pltpu.HBM)
        for array in (density, kernel_factors, jnp.asarray(layout_of(length)[1]))
    ]
    return pl.pallas_call(
        sector_kernel,
        out_shape=pltpu.VMEM(density.shape, f32),
        in_specs=[pl.BlockSpec(memory_space=pl.ANY)] * len(given),
        out_specs=pl.BlockSpec(memory_space=pltpu.VMEM),
        scratch_shapes=[pltpu.VMEM(array.shape, array.dtype) for array in given] + [
            pltpu.VMEM((replicas, 2, tiles, rows_y, length), f32),
            pltpu.VMEM((tiles, length, length), f32),
            pltpu.VMEM((2,) + sheet, f32), pltpu.VMEM(sheet, f32), pltpu.VMEM(sheet, f32),
            pltpu.VMEM((2,) + sheet, f32),
            pltpu.VMEM((half * PITCH, length), f32), pltpu.VMEM((half * PITCH, length), f32),
            pltpu.VMEM((length, length, length), f32),
            pltpu.VMEM(sheet, f32), pltpu.VMEM(sheet, f32), pltpu.VMEM(sheet, f32),
            pltpu.VMEM((2,) + sheet, f32), pltpu.VMEM(sheet, f32),
            pltpu.VMEM((tiles, length, length), f32),
            pltpu.VMEM((replicas, 2, tiles, rows_y, length), f32),
            pltpu.VMEM((3, length, length), f32), pltpu.VMEM((2, length, length), f32),
            pltpu.VMEM((2 * length, 2 * length), bf16),
            pltpu.VMEM((GROUP, 2 * length, 2 * length), bf16),
            dma((6,)), dma((chunks,)), dma((chunks,)), dma((chunks,)),
            dma((chunks,)), dma((chunks,)), dma((replicas, chunks)), dma((5,)),
        ],
        compiler_params=pltpu.CompilerParams(
            has_side_effects=True, vmem_limit_bytes=56 * 2**20, collective_id=0
        ),
    )(*given)


def body(density, kernel_factors):
    replicas, rows_x, rows_y, length = density.shape
    count_px, count_py = lax.axis_size("px"), lax.axis_size("py")
    square = count_px == count_py == 2 * replicas == 4
    whole = rows_x * count_px == rows_y * count_py == length == LANES
    if square and whole and kernel_factors.shape[1] <= LANES:
        return sector_body(density, kernel_factors)
    return plain_body(density, kernel_factors)


def solution(mesh):
    placed = (P("rep", "px", "py", None), P())
    return jax.shard_map(
        body, mesh=mesh, in_specs=placed, out_specs=P("rep", "px", "py", None), check_vma=False
    )
```

```python
import math

import jax
import jax.numpy as jnp
import numpy as np
from jax import lax
from jax.experimental import pallas as pl
from jax.experimental.pallas import tpu as pltpu
from jax.sharding import PartitionSpec as P

HIGHEST = lax.Precision.HIGHEST
LANES = 128
TILES = 2
LAG = 4
LAG_BACK = 3
GROUP = 8
PITCH = 129


def spectral_table(length, chunks):
    freq = np.arange(length).reshape(chunks, 1, length // chunks, 1)
    angle = (freq * np.arange(length) % (2 * length)) * (math.pi / length)
    both = np.concatenate([np.cos(angle), np.sin(angle)], 1)
    return both.reshape(2 * length, length).astype(np.float32)


def dot(spec, left, right):
    return jnp.einsum(spec, left, right, precision=HIGHEST, preferred_element_type=jnp.float32)


def kernel_block(factors, y_start, y_count, z_start, z_count):
    length = factors.shape[2] // 2
    weights = np.full((length,), 1.0 / length, np.float32)
    weights[0] = 0.5 / length
    factors = factors[:, :, :length] * weights
    factor_y = lax.dynamic_slice_in_dim(factors[1], y_start, y_count, 1)
    factor_z = lax.dynamic_slice_in_dim(factors[2], z_start, z_count, 1)
    pair = factor_z[:, :, None] * factor_y[:, None, :]
    return jnp.einsum("gzy,gx->zyx", pair, factors[0], precision=lax.Precision.HIGHEST)


def plain_body(density, kernel_factors):
    replicas, rows_x, rows_y, length = density.shape
    count_px = lax.axis_size("px")
    count_py = lax.axis_size("py")
    half = count_px // replicas
    trade = [[i + half * r for r in range(replicas)] for i in range(half)]
    lines = [[r * half + i for i in range(half)] for r in range(replicas)]
    index_x = lax.axis_index("px") % half
    index_y = lax.axis_index("py")
    table_z = spectral_table(length, count_py)
    table_y = spectral_table(length, half)
    order = np.arange(length).reshape(replicas, half, rows_x).transpose(1, 0, 2).reshape(-1)
    table_x = spectral_table(length, 1)[:, order]

    held = lax.all_to_all(density, "px", 0, 0, axis_index_groups=trade, tiled=True)
    held = held.reshape(replicas * rows_x, rows_y, length)
    held = dot("kz,xyz->kyx", table_z, held)
    held = lax.all_to_all(held, "py", 0, 1, tiled=True)
    held = dot("qy,kyx->kqx", table_y, held)
    held = lax.all_to_all(held, "px", 1, 2, axis_index_groups=lines, tiled=True)
    z_freq, y_freq = length // count_py, length // half
    kernel = kernel_block(kernel_factors, index_x * y_freq, y_freq, index_y * z_freq, z_freq)
    held = dot("kqx,px->kqp", held, table_x)
    held = held.reshape(2, z_freq, 2, y_freq, 2, length) * kernel[None, :, None, :, None, :]
    held = held.reshape(2 * z_freq, 2 * y_freq, 2 * length)
    held = dot("kqp,px->kqx", held, table_x)
    held = lax.all_to_all(held, "px", 2, 1, axis_index_groups=lines, tiled=True)
    held = dot("kqx,qy->kyx", held, table_y)
    held = lax.all_to_all(held, "py", 1, 0, tiled=True)
    held = dot("kyx,kz->xyz", held, table_z)
    held = held.reshape(replicas, rows_x, rows_y, length)
    return lax.all_to_all(held, "px", 0, 0, axis_index_groups=trade, tiled=True)


def halves(values):
    high = values.astype(jnp.bfloat16)
    low = (values - high.astype(jnp.float32)).astype(jnp.bfloat16)
    return high, low


def matmul(left, right):
    return lax.dot_general(left, right, (((1,), (0,)), ((), ())), preferred_element_type=jnp.float32)


def sector_kernel(
    dens_in, factors_in, tables_in, out,
    dens, factors, tables,
    a, z, b, p, swap, x, e, turned_e, kern, keep, c_send, c_held, g, g_send, zr, fin,
    flat, turned, gains, solved,
    sent, sems_z, sems_y, sems_c, sems_ci, sems_yi, sems_zi, sems_in,
):
    replicas, rows_x, rows_y, length = dens.shape
    half = length // 2
    tiles = rows_x // 2
    sizes = [1] * TILES + [TILES] * (tiles // TILES - 2) + [1] * TILES
    coming = [pl.ds(sum(sizes[:i]), size) for i, size in enumerate(sizes)]
    going = [pl.ds(sum(sizes[:i]), size) for i, size in enumerate(sizes)]
    chunks = len(sizes)
    me_px, me_py = lax.axis_index("px"), lax.axis_index("py")
    count_px, count_py = lax.axis_size("px"), lax.axis_size("py")
    side, core = lax.div(me_px, 2), lax.rem(me_px, 2)
    sign = 2 * side - 1
    part = side * (me_px - 2) + (1 - side) * (1 - me_px)
    peers = {1: me_py + 1 - 2 * lax.rem(me_py, 2), 2: lax.rem(me_py + 2, count_py), 3: count_py - 1 - me_py}

    def role(py):
        return lax.div(lax.rem(py + 1, count_py), 2), lax.div(py, 2)

    mine, odd_z = role(me_py)
    outer = mine == 0
    twin = count_px - 1 - me_px
    other = me_px + 1 - 2 * core

    barrier = pltpu.get_barrier_semaphore()
    partners = [{"py": peer} for peer in peers.values()] + [{"px": twin}, {"px": other}]
    for partner in partners:
        pl.semaphore_signal(barrier, inc=1, device_id=partner, device_id_type=pl.DeviceIdType.MESH)

    where_of, _ = layout_of(length)

    def table(name, parity=None):
        start, rows = where_of[name]
        if parity is None:
            return tables[start : start + rows, :]
        rows //= 2
        return tables[pl.ds(pl.multiple_of(start + parity * rows, 16), rows), :]

    loads = {}

    def load(name, src, dst):
        loads[name] = pltpu.make_async_copy(src, dst, sems_in.at[len(loads)])
        loads[name].start()

    early = pl.ds(0, where_of["fold_z"][1])
    late = pl.ds(early.size, tables.shape[0] - early.size)
    load("first", dens_in.at[0], dens.at[0])
    load("fold_z", tables_in.at[early], tables.at[early])
    load("rest", dens_in.at[pl.ds(1, replicas - 1)], dens.at[pl.ds(1, replicas - 1)])
    load("factors", factors_in, factors)
    load("tables", tables_in.at[late], tables.at[late])

    def make(src, dst, stage, sem, device):
        return pltpu.make_async_remote_copy(
            src_ref=src, dst_ref=dst, send_sem=sent.at[stage], recv_sem=sem,
            device_id=device, device_id_type=pl.DeviceIdType.MESH,
        )

    def arrived(ref, sem):
        make(ref, ref, 0, sem, {"px": other}).wait_recv()

    def gone(ref, stage):
        make(ref, ref, stage, sems_y.at[0], {"px": other}).wait_send()

    def lines(py):
        return pl.ds(pl.multiple_of(py * rows_y, 8), rows_y)

    three = pl.ds(0, (count_py - 1) * rows_y)

    def row(tile):
        return side * tile + (1 - side) * (rows_x - 1 - tile)

    def fold(replica, chunk):
        span = coming[chunk]
        left = [dens[replica, row(span.start + i)] for i in range(span.size)]
        right = [dens[replica, row(tiles + span.start + i)] for i in range(span.size)]
        both = jnp.concatenate([jnp.concatenate(left, 0), jnp.concatenate(right, 0)], 1)
        waves = matmul(jnp.concatenate(halves(both), 1), table("fold_z"))
        for parity in range(2):
            cut = waves[:, parity * length : (parity + 1) * length]
            a[replica, parity, span] = cut.reshape(span.size, rows_y, length)

    sends_z = {}
    for chunk in range(chunks):
        for step, peer in peers.items():
            replica, parity = role(peer)
            sends_z[step, chunk] = make(
                a.at[replica, parity, coming[chunk]], z.at[coming[chunk], lines(me_py), :],
                0, sems_z.at[chunk], {"py": peer},
            )

    def steps(replica):
        return ((3,), (2, 1)) if replica == 0 else ((2, 1), (3,))

    def scatter(replica, chunk):
        at_outer, at_inner = steps(replica)

        @pl.when(outer)
        def _():
            for step in at_outer:
                sends_z[step, chunk].start()

        @pl.when(jnp.logical_not(outer))
        def _():
            for step in at_inner:
                sends_z[step, chunk].start()

    loads["first"].wait()
    loads["fold_z"].wait()
    for replica in range(replicas):
        if replica == 1:
            loads["rest"].wait()
        for chunk in range(chunks):
            fold(replica, chunk)
            if replica == chunk == 0:
                pl.semaphore_wait(barrier, len(partners))
            scatter(replica, chunk)

    @pl.loop(0, tiles, unroll=4)
    def _(tile):
        z[tile, lines(me_py), :] = a[mine, odd_z, tile]

    def kernel_setup():
        loads["factors"].wait()
        terms = factors.shape[1]
        flat[...] = jnp.zeros_like(flat)
        where = lax.broadcasted_iota(jnp.int32, (terms, length), 1)
        weight = jnp.where(where == 0, 0.5 / length, 1.0 / length)
        for dim in range(3):
            flat[dim, 0:terms] = factors[dim, :, 0:length] * weight
        for dim in range(2):
            turned[dim] = flat[dim].T
        high, low = halves(flat[2])
        gains[...] = jnp.concatenate(
            [jnp.concatenate([high, low], 1), jnp.concatenate([high, jnp.zeros_like(low)], 1)], 0
        )

    def kernel_values(start, count):
        @pl.loop(start, start + count, unroll=8)
        def _(f):
            pair = turned[0] * turned[1, pl.ds(f, 1), :]
            sums = matmul(jnp.concatenate(halves(pair), 1), gains[...])
            kern[f] = sums[:, :length] + sums[:, length:]

    kernel_setup()
    kernel_values(0, half)

    def fold_lines(chunk):
        span = coming[chunk]
        arrived(z.at[span, three, :], sems_z.at[chunk])
        for tile in range(span.start, span.start + span.size, 2):
            width = min(2, span.start + span.size - tile)
            cells = jnp.concatenate([z[tile + j] for j in range(width)], 1)
            waves = matmul(table("fold_y"), jnp.concatenate(halves(cells), 0))
            for parity in range(2):
                for j in range(width):
                    b[parity, tile + j] = waves[
                        parity * half : (parity + 1) * half, j * length : (j + 1) * length
                    ]
        make(b.at[1 - side, span], p.at[span], 1, sems_y.at[chunk], {"px": twin}).start()

    flip = sign.astype(jnp.float32)
    def fold_sheets(chunk):
        span = coming[chunk]
        arrived(p.at[span], sems_y.at[chunk])
        for tile in range(span.start, span.start + span.size):
            ours, theirs = b[side, tile], p[tile]
            total, gap = ours + theirs, (ours - theirs) * flip
            x[part, tile] = jnp.where(core == 0, total, gap)
            swap[tile] = jnp.where(core == 0, gap, total)
        make(swap.at[span], x.at[part, span], 2, sems_c.at[chunk], {"px": other}).start()

    def forward(pieces):
        cells = [x[where, span].reshape(span.size * half, length) for where, span in pieces]
        high, low = halves(jnp.concatenate(cells, 0))
        waves = matmul(jnp.concatenate([high, low, high], 1), table("wide", odd_z))
        tall = table("tall", side)[:, : 3 * half]
        each = [(where, tile) for where, span in pieces for tile in range(span.start, span.start + span.size)]
        found = []
        for i in range(len(each)):
            high, low = halves(waves[i * half : (i + 1) * half])
            found.append(matmul(tall, jnp.concatenate([high, high, low], 0)))
        for both, (where, tile) in zip(found, each):
            for j in range(2):
                first = (where * rows_x + j * tiles + tile) * PITCH
                e[pl.ds(first, length), :] = both[:, j * length : (j + 1) * length]

    def swapped(chunk):
        arrived(swap.at[coming[chunk]], sems_c.at[chunk])

    loads["tables"].wait()
    for stage in range(chunks + LAG):
        if stage < chunks:
            fold_lines(stage)
        if stage < 4:
            kernel_values(half + stage * half // 4, half // 4)
        if stage >= LAG:
            fold_sheets(stage - LAG)
        ready = stage - LAG - 3
        if ready >= 0 and ready % 2 == 0 and ready < chunks - 4:
            some = coming[ready : ready + 2]
            swapped(ready)
            swapped(ready + 1)
            forward([(where, span) for where in (part, 1 - part) for span in some])
    forward([(part, span) for span in coming[-4:]])
    for chunk in range(chunks - 4, chunks - 1):
        swapped(chunk)
    forward([(1 - part, span) for span in coming[-4:-1]])
    swapped(chunks - 1)
    forward([(1 - part, coming[-1])])

    def spectrum(first):
        cells = jnp.concatenate([e[pl.ds(first + i, half, stride=PITCH), :] for i in range(2)], 1)
        high, low = halves(cells)
        return matmul(table("tall", core)[:, : 3 * half], jnp.concatenate([high, high, low], 0))

    def answer_of(first, k):
        cells = matmul(table("back_tall", core), solved[k])
        cells = cells[:half] + cells[half:]
        for i in range(2):
            turned_e[pl.ds(first + i, half, stride=PITCH), :] = cells[:, i * length : (i + 1) * length]

    def solve(first, k, waves):
        product = waves * jnp.concatenate([kern[first], kern[first + 1]], 1)
        solved[k] = jnp.concatenate(halves(product), 0)

    def middle():
        trips = length // (2 * GROUP)
        for k in range(GROUP):
            solve(2 * k, k, spectrum(2 * k))

        @pl.loop(1, trips)
        def _(f):
            for k in range(GROUP):
                first = 2 * (f * GROUP + k)
                waves = spectrum(first)
                answer_of(first - 2 * GROUP, k)
                solve(first, k, waves)

        for k in range(GROUP):
            answer_of(length - 2 * GROUP + 2 * k, k)

    middle()

    def backward(chunk):
        span = going[chunk]
        rows = []
        for where in (1 - part, part):
            for i in range(span.size):
                cells = []
                for j in range(2):
                    start = (where * rows_x + j * tiles + span.start + i) * PITCH
                    cells.append(turned_e[pl.ds(start, length), :])
                cells = jnp.concatenate(halves(jnp.concatenate(cells, 1)), 0)
                cells = matmul(table("back_tall", side), cells)
                rows.append(cells[:half] + cells[half:])
        high, low = halves(jnp.concatenate(rows, 0))
        wide = table("back_wide", odd_z)
        wide = jnp.concatenate([wide[:, :length], wide[:, length:]], 0)
        cells = matmul(jnp.concatenate([high, low, high], 1), wide)
        found = cells.reshape(2, span.size, half, length)
        c_send[span], keep[span] = found[0], found[1]
        make(c_send.at[span], c_held.at[span], 3, sems_ci.at[chunk], {"px": other}).start()

    def open_sheets(chunk):
        span = going[chunk]
        arrived(c_held.at[span], sems_ci.at[chunk])
        for tile in range(span.start, span.start + span.size):
            first, second = keep[tile], c_held[tile]
            even = jnp.where(core == 0, first, second)
            odd = jnp.where(core == 0, second, first) * flip
            g[side, tile] = even + odd
            g_send[tile] = even - odd
        make(g_send.at[span], g.at[side, span], 4, sems_yi.at[chunk], {"px": twin}).start()

    def answer(step, chunk):
        span = going[chunk]
        return make(
            zr.at[span, lines(peers[step]), :], fin.at[mine, odd_z, span],
            5, sems_zi.at[mine, chunk], {"py": peers[step]},
        )

    def open_lines(chunk):
        span = going[chunk]
        arrived(g_send.at[span], sems_yi.at[chunk])
        for tile in range(span.start, span.start + span.size, 2):
            width = min(2, span.start + span.size - tile)
            both = [
                jnp.concatenate([g[parity, tile + j] for j in range(width)], 1) for parity in range(2)
            ]
            cells = matmul(table("open_y"), jnp.concatenate(halves(jnp.concatenate(both, 0)), 0))
            for j in range(width):
                zr[tile + j] = cells[:, j * length : (j + 1) * length]
        for step in (3, 2):
            answer(step, chunk).start()

        @pl.when(jnp.logical_not(outer))
        def _():
            answer(1, chunk).start()

        fin[mine, odd_z, span] = zr[span, lines(me_py), :]

    for stage in range(chunks + LAG_BACK + 1):
        if stage < chunks:
            backward(stage)
        if 0 <= stage - 1 < chunks:
            open_sheets(stage - 1)
        if 0 <= stage - LAG_BACK - 1:
            open_lines(stage - LAG_BACK - 1)

    @pl.when(outer)
    def _():
        for chunk in range(chunks):
            answer(1, chunk).start()

    for stage, ref in enumerate((z.at[:, three, :], p, swap, c_send, g_send)):
        gone(ref, stage)

    def finish(replica, chunk):
        span = going[chunk]
        few, many = (outer, jnp.logical_not(outer))[:: 1 - 2 * replica]

        @pl.when(few)
        def _():
            arrived(fin.at[replica, 0, span], sems_zi.at[replica, chunk])

        @pl.when(many)
        def _():
            arrived(fin.at[replica, :, span], sems_zi.at[replica, chunk])

        both = [fin[replica, parity, span].reshape(span.size * rows_y, length) for parity in range(2)]
        cells = matmul(jnp.concatenate(halves(jnp.concatenate(both, 1)), 1), table("open_z"))
        for i in range(span.size):
            cut = cells[i * rows_y : (i + 1) * rows_y]
            out[replica, row(span.start + i)] = cut[:, :length]
            out[replica, row(tiles + span.start + i)] = cut[:, length:]

    for replica in range(replicas):
        for chunk in range(chunks):
            if replica == 1 and chunk == chunks - 1:
                gone(zr.at[:, three, :], 5)
            finish(replica, chunk)


def twice(table):
    zero = np.zeros_like(table)
    return np.block([[table, zero], [zero, table]])


def tables_of(length):
    half = length // 2
    angle = (np.arange(length)[:, None] * (2 * np.arange(half) + 1) % (4 * length)) * (math.pi / (2 * length))
    waves = np.stack([np.cos(angle), np.sin(angle)]).astype(np.float32)
    high = waves.astype(jnp.bfloat16).astype(np.float32)
    low = waves - high
    near, far = np.eye(half), np.eye(half)[::-1]
    line = np.block([[far, near], [-far, near]])
    sides = [line[:half].T, line[half:].T]
    fold_z = np.concatenate([twice(side) for side in sides], 1)
    fold_z = np.concatenate([fold_z, fold_z], 0)
    fold_y = np.concatenate([line, line], 1)
    open_y = np.concatenate([line.T, line.T], 1)
    open_z = np.concatenate([twice(side.T) for side in sides], 0)
    open_z = np.concatenate([open_z, open_z], 0)
    wide, tall, back_tall, back_wide = [], [], [], []
    for parity in range(2):
        up, down = high[parity], low[parity]
        wide.append(np.concatenate([twice(up.T), twice(up.T), twice(down.T)], 0))
        tall.append(np.concatenate([up, down, up], 1))
        back_tall.append(np.block([[up.T, up.T], [down.T, np.zeros_like(down.T)]]))
        back_wide.append(np.concatenate([twice(up), twice(up), twice(down)], 0))
    tall = np.concatenate(tall, 0)
    back_wide = [np.concatenate(np.split(one, 2, 0), 1) for one in back_wide]
    found = {
        "fold_z": fold_z, "fold_y": fold_y, "wide": np.concatenate(wide, 0),
        "tall": np.pad(tall, ((0, 0), (0, 2 * length - tall.shape[1]))),
        "back_tall": np.concatenate(back_tall, 0), "back_wide": np.concatenate(back_wide, 0),
        "open_y": open_y, "open_z": open_z,
    }
    return {name: one.astype(np.float32).astype(jnp.bfloat16) for name, one in found.items()}


def layout_of(length):
    found, start = {}, 0
    tables = tables_of(length)
    for name, one in tables.items():
        found[name] = (start, one.shape[0])
        start += one.shape[0]
    return found, np.concatenate(list(tables.values()), 0)


def sector_body(density, kernel_factors):
    replicas, rows_x, rows_y, length = density.shape
    half, tiles = length // 2, rows_x // 2
    chunks = tiles // TILES - 2 + 2 * TILES
    f32, bf16 = jnp.float32, jnp.bfloat16
    dma = pltpu.SemaphoreType.DMA
    sheet = (tiles, half, length)
    given = [
        pltpu.with_memory_space_constraint(array, pltpu.HBM)
        for array in (density, kernel_factors, jnp.asarray(layout_of(length)[1]))
    ]
    return pl.pallas_call(
        sector_kernel,
        out_shape=pltpu.VMEM(density.shape, f32),
        in_specs=[pl.BlockSpec(memory_space=pl.ANY)] * len(given),
        out_specs=pl.BlockSpec(memory_space=pltpu.VMEM),
        scratch_shapes=[pltpu.VMEM(array.shape, array.dtype) for array in given] + [
            pltpu.VMEM((replicas, 2, tiles, rows_y, length), f32),
            pltpu.VMEM((tiles, length, length), f32),
            pltpu.VMEM((2,) + sheet, f32), pltpu.VMEM(sheet, f32), pltpu.VMEM(sheet, f32),
            pltpu.VMEM((2,) + sheet, f32),
            pltpu.VMEM((half * PITCH, length), f32), pltpu.VMEM((half * PITCH, length), f32),
            pltpu.VMEM((length, length, length), f32),
            pltpu.VMEM(sheet, f32), pltpu.VMEM(sheet, f32), pltpu.VMEM(sheet, f32),
            pltpu.VMEM((2,) + sheet, f32), pltpu.VMEM(sheet, f32),
            pltpu.VMEM((tiles, length, length), f32),
            pltpu.VMEM((replicas, 2, tiles, rows_y, length), f32),
            pltpu.VMEM((3, length, length), f32), pltpu.VMEM((2, length, length), f32),
            pltpu.VMEM((2 * length, 2 * length), bf16),
            pltpu.VMEM((GROUP, 2 * length, 2 * length), bf16),
            dma((6,)), dma((chunks,)), dma((chunks,)), dma((chunks,)),
            dma((chunks,)), dma((chunks,)), dma((replicas, chunks)), dma((5,)),
        ],
        compiler_params=pltpu.CompilerParams(
            has_side_effects=True, vmem_limit_bytes=56 * 2**20, collective_id=0
        ),
    )(*given)


def body(density, kernel_factors):
    replicas, rows_x, rows_y, length = density.shape
    count_px, count_py = lax.axis_size("px"), lax.axis_size("py")
    square = count_px == count_py == 2 * replicas == 4
    whole = rows_x * count_px == rows_y * count_py == length == LANES
    if square and whole and kernel_factors.shape[1] <= LANES:
        return sector_body(density, kernel_factors)
    return plain_body(density, kernel_factors)


def solution(mesh):
    placed = (P("rep", "px", "py", None), P())
    return jax.shard_map(
        body, mesh=mesh, in_specs=placed, out_specs=P("rep", "px", "py", None), check_vma=False
    )
```

```python
import math

import jax
import jax.numpy as jnp
import numpy as np
from jax import lax
from jax.experimental import pallas as pl
from jax.experimental.pallas import tpu as pltpu
from jax.sharding import PartitionSpec as P

HIGHEST = lax.Precision.HIGHEST
LANES = 128
TILES = 2
LAG = 4
LAG_BACK = 3
GROUP = 16
PITCH = 129


def spectral_table(length, chunks):
    freq = np.arange(length).reshape(chunks, 1, length // chunks, 1)
    angle = (freq * np.arange(length) % (2 * length)) * (math.pi / length)
    both = np.concatenate([np.cos(angle), np.sin(angle)], 1)
    return both.reshape(2 * length, length).astype(np.float32)


def dot(spec, left, right):
    return jnp.einsum(spec, left, right, precision=HIGHEST, preferred_element_type=jnp.float32)


def kernel_block(factors, y_start, y_count, z_start, z_count):
    length = factors.shape[2] // 2
    weights = np.full((length,), 1.0 / length, np.float32)
    weights[0] = 0.5 / length
    factors = factors[:, :, :length] * weights
    factor_y = lax.dynamic_slice_in_dim(factors[1], y_start, y_count, 1)
    factor_z = lax.dynamic_slice_in_dim(factors[2], z_start, z_count, 1)
    pair = factor_z[:, :, None] * factor_y[:, None, :]
    return jnp.einsum("gzy,gx->zyx", pair, factors[0], precision=lax.Precision.HIGHEST)


def plain_body(density, kernel_factors):
    replicas, rows_x, rows_y, length = density.shape
    count_px = lax.axis_size("px")
    count_py = lax.axis_size("py")
    half = count_px // replicas
    trade = [[i + half * r for r in range(replicas)] for i in range(half)]
    lines = [[r * half + i for i in range(half)] for r in range(replicas)]
    index_x = lax.axis_index("px") % half
    index_y = lax.axis_index("py")
    table_z = spectral_table(length, count_py)
    table_y = spectral_table(length, half)
    order = np.arange(length).reshape(replicas, half, rows_x).transpose(1, 0, 2).reshape(-1)
    table_x = spectral_table(length, 1)[:, order]

    held = lax.all_to_all(density, "px", 0, 0, axis_index_groups=trade, tiled=True)
    held = held.reshape(replicas * rows_x, rows_y, length)
    held = dot("kz,xyz->kyx", table_z, held)
    held = lax.all_to_all(held, "py", 0, 1, tiled=True)
    held = dot("qy,kyx->kqx", table_y, held)
    held = lax.all_to_all(held, "px", 1, 2, axis_index_groups=lines, tiled=True)
    z_freq, y_freq = length // count_py, length // half
    kernel = kernel_block(kernel_factors, index_x * y_freq, y_freq, index_y * z_freq, z_freq)
    held = dot("kqx,px->kqp", held, table_x)
    held = held.reshape(2, z_freq, 2, y_freq, 2, length) * kernel[None, :, None, :, None, :]
    held = held.reshape(2 * z_freq, 2 * y_freq, 2 * length)
    held = dot("kqp,px->kqx", held, table_x)
    held = lax.all_to_all(held, "px", 2, 1, axis_index_groups=lines, tiled=True)
    held = dot("kqx,qy->kyx", held, table_y)
    held = lax.all_to_all(held, "py", 1, 0, tiled=True)
    held = dot("kyx,kz->xyz", held, table_z)
    held = held.reshape(replicas, rows_x, rows_y, length)
    return lax.all_to_all(held, "px", 0, 0, axis_index_groups=trade, tiled=True)


def halves(values):
    high = values.astype(jnp.bfloat16)
    low = (values - high.astype(jnp.float32)).astype(jnp.bfloat16)
    return high, low


def matmul(left, right):
    return lax.dot_general(left, right, (((1,), (0,)), ((), ())), preferred_element_type=jnp.float32)


def sector_kernel(
    dens_in, factors_in, tables_in, out,
    dens, factors, tables,
    a, z, b, p, swap, x, e, turned_e, kern, keep, c_send, c_held, g, g_send, zr, fin,
    flat, turned, gains, solved,
    sent, sems_z, sems_y, sems_c, sems_ci, sems_yi, sems_zi, sems_in,
):
    replicas, rows_x, rows_y, length = dens.shape
    half = length // 2
    tiles = rows_x // 2
    sizes = [1] * TILES + [TILES] * (tiles // TILES - 2) + [1] * TILES
    coming = [pl.ds(sum(sizes[:i]), size) for i, size in enumerate(sizes)]
    going = [pl.ds(sum(sizes[:i]), size) for i, size in enumerate(sizes)]
    chunks = len(sizes)
    me_px, me_py = lax.axis_index("px"), lax.axis_index("py")
    count_px, count_py = lax.axis_size("px"), lax.axis_size("py")
    side, core = lax.div(me_px, 2), lax.rem(me_px, 2)
    sign = 2 * side - 1
    part = side * (me_px - 2) + (1 - side) * (1 - me_px)
    peers = {1: me_py + 1 - 2 * lax.rem(me_py, 2), 2: lax.rem(me_py + 2, count_py), 3: count_py - 1 - me_py}

    def role(py):
        return lax.div(lax.rem(py + 1, count_py), 2), lax.div(py, 2)

    mine, odd_z = role(me_py)
    outer = mine == 0
    inner = jnp.logical_not(outer)
    twin = count_px - 1 - me_px
    other = me_px + 1 - 2 * core

    barrier = pltpu.get_barrier_semaphore()
    partners = [{"py": peer} for peer in peers.values()] + [{"px": twin}, {"px": other}]
    for partner in partners:
        pl.semaphore_signal(barrier, inc=1, device_id=partner, device_id_type=pl.DeviceIdType.MESH)

    where_of, _ = layout_of(length)

    def table(name, parity=None):
        start, rows = where_of[name]
        if parity is None:
            return tables[start : start + rows, :]
        rows //= 2
        return tables[pl.ds(pl.multiple_of(start + parity * rows, 16), rows), :]

    loads = {}

    def load(name, src, dst):
        loads[name] = pltpu.make_async_copy(src, dst, sems_in.at[len(loads)])
        loads[name].start()

    early = pl.ds(0, where_of["fold_z"][1])
    late = pl.ds(early.size, tables.shape[0] - early.size)
    load("first", dens_in.at[0], dens.at[0])
    load("fold_z", tables_in.at[early], tables.at[early])
    load("rest", dens_in.at[pl.ds(1, replicas - 1)], dens.at[pl.ds(1, replicas - 1)])
    load("factors", factors_in, factors)
    load("tables", tables_in.at[late], tables.at[late])

    def make(src, dst, stage, sem, device):
        return pltpu.make_async_remote_copy(
            src_ref=src, dst_ref=dst, send_sem=sent.at[stage], recv_sem=sem,
            device_id=device, device_id_type=pl.DeviceIdType.MESH,
        )

    def arrived(ref, sem):
        make(ref, ref, 0, sem, {"px": other}).wait_recv()

    def gone(ref, stage):
        make(ref, ref, stage, sems_y.at[0], {"px": other}).wait_send()

    def lines(py):
        return pl.ds(pl.multiple_of(py * rows_y, 8), rows_y)

    three = pl.ds(0, (count_py - 1) * rows_y)

    def row(tile):
        return side * tile + (1 - side) * (rows_x - 1 - tile)

    def fold(replica, chunk):
        span = coming[chunk]
        left = [dens[replica, row(span.start + i)] for i in range(span.size)]
        right = [dens[replica, row(tiles + span.start + i)] for i in range(span.size)]
        both = jnp.concatenate([jnp.concatenate(left, 0), jnp.concatenate(right, 0)], 1)
        waves = matmul(jnp.concatenate(halves(both), 1), table("fold_z"))
        for parity in range(2):
            cut = waves[:, parity * length : (parity + 1) * length]
            a[replica, parity, span] = cut.reshape(span.size, rows_y, length)

    sends_z = {}
    for chunk in range(chunks):
        for step, peer in peers.items():
            replica, parity = role(peer)
            sends_z[step, chunk] = make(
                a.at[replica, parity, coming[chunk]], z.at[coming[chunk], lines(me_py), :],
                0, sems_z.at[chunk], {"py": peer},
            )

    def steps(replica):
        return ((3,), (2, 1)) if replica == 0 else ((2, 1), (3,))

    def scatter(replica, chunk):
        at_outer, at_inner = steps(replica)

        @pl.when(outer)
        def _():
            for step in at_outer:
                sends_z[step, chunk].start()

        @pl.when(jnp.logical_not(outer))
        def _():
            for step in at_inner:
                sends_z[step, chunk].start()

    loads["first"].wait()
    loads["fold_z"].wait()
    for replica in range(replicas):
        if replica == 1:
            loads["rest"].wait()
        for chunk in range(chunks):
            fold(replica, chunk)
            if replica == chunk == 0:
                pl.semaphore_wait(barrier, len(partners))
            scatter(replica, chunk)

    @pl.loop(0, tiles, unroll=4)
    def _(tile):
        z[tile, lines(me_py), :] = a[mine, odd_z, tile]

    def kernel_setup():
        loads["factors"].wait()
        terms = factors.shape[1]
        flat[...] = jnp.zeros_like(flat)
        where = lax.broadcasted_iota(jnp.int32, (terms, length), 1)
        weight = jnp.where(where == 0, 0.5 / length, 1.0 / length)
        for dim in range(3):
            flat[dim, 0:terms] = factors[dim, :, 0:length] * weight
        for dim in range(2):
            turned[dim] = flat[dim].T
        high, low = halves(flat[2])
        gains[...] = jnp.concatenate(
            [jnp.concatenate([high, low], 1), jnp.concatenate([high, jnp.zeros_like(low)], 1)], 0
        )

    def kernel_values(start, count):
        @pl.loop(start, start + count, unroll=8)
        def _(f):
            pair = turned[0] * turned[1, pl.ds(f, 1), :]
            sums = matmul(jnp.concatenate(halves(pair), 1), gains[...])
            kern[f] = sums[:, :length] + sums[:, length:]

    kernel_setup()
    kernel_values(0, half)

    def fold_lines(chunk):
        span = coming[chunk]
        arrived(z.at[span, three, :], sems_z.at[chunk])
        for tile in range(span.start, span.start + span.size, 2):
            width = min(2, span.start + span.size - tile)
            cells = jnp.concatenate([z[tile + j] for j in range(width)], 1)
            waves = matmul(table("fold_y"), jnp.concatenate(halves(cells), 0))
            for parity in range(2):
                for j in range(width):
                    b[parity, tile + j] = waves[
                        parity * half : (parity + 1) * half, j * length : (j + 1) * length
                    ]
        make(b.at[1 - side, span], p.at[span], 1, sems_y.at[chunk], {"px": twin}).start()

    flip = sign.astype(jnp.float32)
    def fold_sheets(chunk):
        span = coming[chunk]
        arrived(p.at[span], sems_y.at[chunk])
        for tile in range(span.start, span.start + span.size):
            ours, theirs = b[side, tile], p[tile]
            total, gap = ours + theirs, (ours - theirs) * flip
            x[part, tile] = jnp.where(core == 0, total, gap)
            swap[tile] = jnp.where(core == 0, gap, total)
        make(swap.at[span], x.at[part, span], 2, sems_c.at[chunk], {"px": other}).start()

    def forward(pieces):
        cells = [x[where, span].reshape(span.size * half, length) for where, span in pieces]
        high, low = halves(jnp.concatenate(cells, 0))
        waves = matmul(jnp.concatenate([high, low, high], 1), table("wide", odd_z))
        tall = table("tall", side)[:, : 3 * half]
        each = [(where, tile) for where, span in pieces for tile in range(span.start, span.start + span.size)]
        found = []
        for i in range(len(each)):
            high, low = halves(waves[i * half : (i + 1) * half])
            found.append(matmul(tall, jnp.concatenate([high, high, low], 0)))
        for both, (where, tile) in zip(found, each):
            for j in range(2):
                first = (where * rows_x + j * tiles + tile) * PITCH
                e[pl.ds(first, length), :] = both[:, j * length : (j + 1) * length]

    def swapped(chunk):
        arrived(swap.at[coming[chunk]], sems_c.at[chunk])

    loads["tables"].wait()
    for stage in range(chunks + LAG):
        if stage < chunks:
            fold_lines(stage)
        if stage < 4:
            kernel_values(half + stage * half // 4, half // 4)
        if stage >= LAG:
            fold_sheets(stage - LAG)
        ready = stage - LAG - 3
        if ready >= 0 and ready % 2 == 0 and ready < chunks - 4:
            some = coming[ready : ready + 2]
            swapped(ready)
            swapped(ready + 1)
            forward([(where, span) for where in (part, 1 - part) for span in some])
    forward([(part, span) for span in coming[-4:]])
    for chunk in range(chunks - 4, chunks - 1):
        swapped(chunk)
    forward([(1 - part, span) for span in coming[-4:-1]])
    swapped(chunks - 1)
    forward([(1 - part, coming[-1])])

    def spectrum(first):
        cells = jnp.concatenate([e[pl.ds(first + i, half, stride=PITCH), :] for i in range(2)], 1)
        high, low = halves(cells)
        return matmul(table("tall", core)[:, : 3 * half], jnp.concatenate([high, high, low], 0))

    def answer_of(first, k):
        cells = matmul(table("back_tall", core), solved[k])
        cells = cells[:half] + cells[half:]
        for i in range(2):
            turned_e[pl.ds(first + i, half, stride=PITCH), :] = cells[:, i * length : (i + 1) * length]

    def solve(first, k, waves):
        product = waves * jnp.concatenate([kern[first], kern[first + 1]], 1)
        solved[k] = jnp.concatenate(halves(product), 0)

    def middle():
        trips = length // (2 * GROUP)
        for k in range(GROUP):
            solve(2 * k, k, spectrum(2 * k))

        @pl.loop(1, trips)
        def _(f):
            for k in range(GROUP):
                first = 2 * (f * GROUP + k)
                waves = spectrum(first)
                answer_of(first - 2 * GROUP, k)
                solve(first, k, waves)

        for k in range(GROUP):
            answer_of(length - 2 * GROUP + 2 * k, k)

    middle()

    def backward(chunk):
        span = going[chunk]
        rows = []
        for where in (1 - part, part):
            for i in range(span.size):
                cells = []
                for j in range(2):
                    start = (where * rows_x + j * tiles + span.start + i) * PITCH
                    cells.append(turned_e[pl.ds(start, length), :])
                cells = jnp.concatenate(halves(jnp.concatenate(cells, 1)), 0)
                cells = matmul(table("back_tall", side), cells)
                rows.append(cells[:half] + cells[half:])
        high, low = halves(jnp.concatenate(rows, 0))
        wide = table("back_wide", odd_z)
        wide = jnp.concatenate([wide[:, :length], wide[:, length:]], 0)
        cells = matmul(jnp.concatenate([high, low, high], 1), wide)
        found = cells.reshape(2, span.size, half, length)
        c_send[span], keep[span] = found[0], found[1]
        make(c_send.at[span], c_held.at[span], 3, sems_ci.at[chunk], {"px": other}).start()

    def open_sheets(chunk):
        span = going[chunk]
        arrived(c_held.at[span], sems_ci.at[chunk])
        for tile in range(span.start, span.start + span.size):
            first, second = keep[tile], c_held[tile]
            even = jnp.where(core == 0, first, second)
            odd = jnp.where(core == 0, second, first) * flip
            g[side, tile] = even + odd
            g_send[tile] = even - odd
        make(g_send.at[span], g.at[side, span], 4, sems_yi.at[chunk], {"px": twin}).start()

    def answer(step, chunk):
        span = going[chunk]
        return make(
            zr.at[span, lines(peers[step]), :], fin.at[mine, odd_z, span],
            5, sems_zi.at[mine * (chunk + 1)], {"py": peers[step]},
        )

    def open_lines(chunk):
        span = going[chunk]
        arrived(g_send.at[span], sems_yi.at[chunk])
        for tile in range(span.start, span.start + span.size, 2):
            width = min(2, span.start + span.size - tile)
            both = [
                jnp.concatenate([g[parity, tile + j] for j in range(width)], 1) for parity in range(2)
            ]
            cells = matmul(table("open_y"), jnp.concatenate(halves(jnp.concatenate(both, 0)), 0))
            for j in range(width):
                zr[tile + j] = cells[:, j * length : (j + 1) * length]
        for step in (3, 2):
            answer(step, chunk).start()

        @pl.when(jnp.logical_not(outer))
        def _():
            answer(1, chunk).start()

        fin[mine, odd_z, span] = zr[span, lines(me_py), :]

    for stage in range(chunks + LAG_BACK + 1):
        if stage < chunks:
            backward(stage)
        if 0 <= stage - 1 < chunks:
            open_sheets(stage - 1)
        if 0 <= stage - LAG_BACK - 1:
            open_lines(stage - LAG_BACK - 1)

    @pl.when(outer)
    def _():
        for chunk in range(chunks):
            answer(1, chunk).start()

    for stage, ref in enumerate((z.at[:, three, :], p, swap, c_send, g_send)):
        gone(ref, stage)

    def collect(replica, span, sem):
        few, many = (outer, inner)[:: 1 - 2 * replica]

        @pl.when(few)
        def _():
            arrived(fin.at[replica, 0, span], sem)

        @pl.when(many)
        def _():
            arrived(fin.at[replica, :, span], sem)

    def finish(replica, chunk):
        span = going[chunk]
        if replica == 1:
            collect(replica, span, sems_zi.at[chunk + 1])
        both = [fin[replica, parity, span].reshape(span.size * rows_y, length) for parity in range(2)]
        cells = matmul(jnp.concatenate(halves(jnp.concatenate(both, 1)), 1), table("open_z"))
        for i in range(span.size):
            cut = cells[i * rows_y : (i + 1) * rows_y]
            out[replica, row(span.start + i)] = cut[:, :length]
            out[replica, row(tiles + span.start + i)] = cut[:, length:]

    collect(0, pl.ds(0, tiles), sems_zi.at[0])
    for replica in range(replicas):
        for chunk in range(chunks):
            if replica == 1 and chunk == chunks - 1:
                gone(zr.at[:, three, :], 5)
            finish(replica, chunk)


def twice(table):
    zero = np.zeros_like(table)
    return np.block([[table, zero], [zero, table]])


def tables_of(length):
    half = length // 2
    angle = (np.arange(length)[:, None] * (2 * np.arange(half) + 1) % (4 * length)) * (math.pi / (2 * length))
    waves = np.stack([np.cos(angle), np.sin(angle)]).astype(np.float32)
    high = waves.astype(jnp.bfloat16).astype(np.float32)
    low = waves - high
    near, far = np.eye(half), np.eye(half)[::-1]
    line = np.block([[far, near], [-far, near]])
    sides = [line[:half].T, line[half:].T]
    fold_z = np.concatenate([twice(side) for side in sides], 1)
    fold_z = np.concatenate([fold_z, fold_z], 0)
    fold_y = np.concatenate([line, line], 1)
    open_y = np.concatenate([line.T, line.T], 1)
    open_z = np.concatenate([twice(side.T) for side in sides], 0)
    open_z = np.concatenate([open_z, open_z], 0)
    wide, tall, back_tall, back_wide = [], [], [], []
    for parity in range(2):
        up, down = high[parity], low[parity]
        wide.append(np.concatenate([twice(up.T), twice(up.T), twice(down.T)], 0))
        tall.append(np.concatenate([up, down, up], 1))
        back_tall.append(np.block([[up.T, up.T], [down.T, np.zeros_like(down.T)]]))
        back_wide.append(np.concatenate([twice(up), twice(up), twice(down)], 0))
    tall = np.concatenate(tall, 0)
    back_wide = [np.concatenate(np.split(one, 2, 0), 1) for one in back_wide]
    found = {
        "fold_z": fold_z, "fold_y": fold_y, "wide": np.concatenate(wide, 0),
        "tall": np.pad(tall, ((0, 0), (0, 2 * length - tall.shape[1]))),
        "back_tall": np.concatenate(back_tall, 0), "back_wide": np.concatenate(back_wide, 0),
        "open_y": open_y, "open_z": open_z,
    }
    return {name: one.astype(np.float32).astype(jnp.bfloat16) for name, one in found.items()}


def layout_of(length):
    found, start = {}, 0
    tables = tables_of(length)
    for name, one in tables.items():
        found[name] = (start, one.shape[0])
        start += one.shape[0]
    return found, np.concatenate(list(tables.values()), 0)


def sector_body(density, kernel_factors):
    replicas, rows_x, rows_y, length = density.shape
    half, tiles = length // 2, rows_x // 2
    chunks = tiles // TILES - 2 + 2 * TILES
    f32, bf16 = jnp.float32, jnp.bfloat16
    dma = pltpu.SemaphoreType.DMA
    sheet = (tiles, half, length)
    given = [
        pltpu.with_memory_space_constraint(array, pltpu.HBM)
        for array in (density, kernel_factors, jnp.asarray(layout_of(length)[1]))
    ]
    return pl.pallas_call(
        sector_kernel,
        out_shape=pltpu.VMEM(density.shape, f32),
        in_specs=[pl.BlockSpec(memory_space=pl.ANY)] * len(given),
        out_specs=pl.BlockSpec(memory_space=pltpu.VMEM),
        scratch_shapes=[pltpu.VMEM(array.shape, array.dtype) for array in given] + [
            pltpu.VMEM((replicas, 2, tiles, rows_y, length), f32),
            pltpu.VMEM((tiles, length, length), f32),
            pltpu.VMEM((2,) + sheet, f32), pltpu.VMEM(sheet, f32), pltpu.VMEM(sheet, f32),
            pltpu.VMEM((2,) + sheet, f32),
            pltpu.VMEM((half * PITCH, length), f32), pltpu.VMEM((half * PITCH, length), f32),
            pltpu.VMEM((length, length, length), f32),
            pltpu.VMEM(sheet, f32), pltpu.VMEM(sheet, f32), pltpu.VMEM(sheet, f32),
            pltpu.VMEM((2,) + sheet, f32), pltpu.VMEM(sheet, f32),
            pltpu.VMEM((tiles, length, length), f32),
            pltpu.VMEM((replicas, 2, tiles, rows_y, length), f32),
            pltpu.VMEM((3, length, length), f32), pltpu.VMEM((2, length, length), f32),
            pltpu.VMEM((2 * length, 2 * length), bf16),
            pltpu.VMEM((GROUP, 2 * length, 2 * length), bf16),
            dma((6,)), dma((chunks,)), dma((chunks,)), dma((chunks,)),
            dma((chunks,)), dma((chunks,)), dma((chunks + 1,)), dma((5,)),
        ],
        compiler_params=pltpu.CompilerParams(
            has_side_effects=True, vmem_limit_bytes=56 * 2**20, collective_id=0
        ),
    )(*given)


def body(density, kernel_factors):
    replicas, rows_x, rows_y, length = density.shape
    count_px, count_py = lax.axis_size("px"), lax.axis_size("py")
    square = count_px == count_py == 2 * replicas == 4
    whole = rows_x * count_px == rows_y * count_py == length == LANES
    if square and whole and kernel_factors.shape[1] <= LANES:
        return sector_body(density, kernel_factors)
    return plain_body(density, kernel_factors)


def solution(mesh):
    placed = (P("rep", "px", "py", None), P())
    return jax.shard_map(
        body, mesh=mesh, in_specs=placed, out_specs=P("rep", "px", "py", None), check_vma=False
    )
```

```python
import math

import jax
import jax.numpy as jnp
import numpy as np
from jax import lax
from jax.experimental import pallas as pl
from jax.experimental.pallas import tpu as pltpu
from jax.sharding import PartitionSpec as P

HIGHEST = lax.Precision.HIGHEST
LANES = 128
TILES = 2
LAG = 4
LAG_BACK = 3
GROUP = 32
PITCH = 129


def spectral_table(length, chunks):
    freq = np.arange(length).reshape(chunks, 1, length // chunks, 1)
    angle = (freq * np.arange(length) % (2 * length)) * (math.pi / length)
    both = np.concatenate([np.cos(angle), np.sin(angle)], 1)
    return both.reshape(2 * length, length).astype(np.float32)


def dot(spec, left, right):
    return jnp.einsum(spec, left, right, precision=HIGHEST, preferred_element_type=jnp.float32)


def kernel_block(factors, y_start, y_count, z_start, z_count):
    length = factors.shape[2] // 2
    weights = np.full((length,), 1.0 / length, np.float32)
    weights[0] = 0.5 / length
    factors = factors[:, :, :length] * weights
    factor_y = lax.dynamic_slice_in_dim(factors[1], y_start, y_count, 1)
    factor_z = lax.dynamic_slice_in_dim(factors[2], z_start, z_count, 1)
    pair = factor_z[:, :, None] * factor_y[:, None, :]
    return jnp.einsum("gzy,gx->zyx", pair, factors[0], precision=lax.Precision.HIGHEST)


def plain_body(density, kernel_factors):
    replicas, rows_x, rows_y, length = density.shape
    count_px = lax.axis_size("px")
    count_py = lax.axis_size("py")
    half = count_px // replicas
    trade = [[i + half * r for r in range(replicas)] for i in range(half)]
    lines = [[r * half + i for i in range(half)] for r in range(replicas)]
    index_x = lax.axis_index("px") % half
    index_y = lax.axis_index("py")
    table_z = spectral_table(length, count_py)
    table_y = spectral_table(length, half)
    order = np.arange(length).reshape(replicas, half, rows_x).transpose(1, 0, 2).reshape(-1)
    table_x = spectral_table(length, 1)[:, order]

    held = lax.all_to_all(density, "px", 0, 0, axis_index_groups=trade, tiled=True)
    held = held.reshape(replicas * rows_x, rows_y, length)
    held = dot("kz,xyz->kyx", table_z, held)
    held = lax.all_to_all(held, "py", 0, 1, tiled=True)
    held = dot("qy,kyx->kqx", table_y, held)
    held = lax.all_to_all(held, "px", 1, 2, axis_index_groups=lines, tiled=True)
    z_freq, y_freq = length // count_py, length // half
    kernel = kernel_block(kernel_factors, index_x * y_freq, y_freq, index_y * z_freq, z_freq)
    held = dot("kqx,px->kqp", held, table_x)
    held = held.reshape(2, z_freq, 2, y_freq, 2, length) * kernel[None, :, None, :, None, :]
    held = held.reshape(2 * z_freq, 2 * y_freq, 2 * length)
    held = dot("kqp,px->kqx", held, table_x)
    held = lax.all_to_all(held, "px", 2, 1, axis_index_groups=lines, tiled=True)
    held = dot("kqx,qy->kyx", held, table_y)
    held = lax.all_to_all(held, "py", 1, 0, tiled=True)
    held = dot("kyx,kz->xyz", held, table_z)
    held = held.reshape(replicas, rows_x, rows_y, length)
    return lax.all_to_all(held, "px", 0, 0, axis_index_groups=trade, tiled=True)


def halves(values):
    high = values.astype(jnp.bfloat16)
    low = (values - high.astype(jnp.float32)).astype(jnp.bfloat16)
    return high, low


def matmul(left, right):
    return lax.dot_general(left, right, (((1,), (0,)), ((), ())), preferred_element_type=jnp.float32)


def sector_kernel(
    dens_in, factors_in, tables_in, out,
    dens, factors, tables,
    a, z, b, p, swap, x, e, turned_e, kern, keep, c_send, c_held, g, g_send, zr, fin,
    flat, turned, gains, solved,
    sent, sems_z, sems_y, sems_c, sems_ci, sems_yi, sems_zi, sems_in,
):
    replicas, rows_x, rows_y, length = dens.shape
    half = length // 2
    tiles = rows_x // 2
    sizes = [1] * TILES + [TILES] * (tiles // TILES - 2) + [1] * TILES
    coming = [pl.ds(sum(sizes[:i]), size) for i, size in enumerate(sizes)]
    going = [pl.ds(sum(sizes[:i]), size) for i, size in enumerate(sizes)]
    chunks = len(sizes)
    me_px, me_py = lax.axis_index("px"), lax.axis_index("py")
    count_px, count_py = lax.axis_size("px"), lax.axis_size("py")
    side, core = lax.div(me_px, 2), lax.rem(me_px, 2)
    sign = 2 * side - 1
    part = side * (me_px - 2) + (1 - side) * (1 - me_px)
    peers = {1: me_py + 1 - 2 * lax.rem(me_py, 2), 2: lax.rem(me_py + 2, count_py), 3: count_py - 1 - me_py}

    def role(py):
        return lax.div(lax.rem(py + 1, count_py), 2), lax.div(py, 2)

    mine, odd_z = role(me_py)
    outer = mine == 0
    inner = jnp.logical_not(outer)
    twin = count_px - 1 - me_px
    other = me_px + 1 - 2 * core

    barrier = pltpu.get_barrier_semaphore()
    partners = [{"py": peer} for peer in peers.values()] + [{"px": twin}, {"px": other}]
    for partner in partners:
        pl.semaphore_signal(barrier, inc=1, device_id=partner, device_id_type=pl.DeviceIdType.MESH)

    where_of, _ = layout_of(length)

    def table(name, parity=None):
        start, rows = where_of[name]
        if parity is None:
            return tables[start : start + rows, :]
        rows //= 2
        return tables[pl.ds(pl.multiple_of(start + parity * rows, 16), rows), :]

    loads = {}

    def load(name, src, dst):
        loads[name] = pltpu.make_async_copy(src, dst, sems_in.at[len(loads)])
        loads[name].start()

    early = pl.ds(0, where_of["fold_z"][1])
    late = pl.ds(early.size, tables.shape[0] - early.size)
    load("first", dens_in.at[0], dens.at[0])
    load("fold_z", tables_in.at[early], tables.at[early])
    load("rest", dens_in.at[pl.ds(1, replicas - 1)], dens.at[pl.ds(1, replicas - 1)])
    load("factors", factors_in, factors)
    load("tables", tables_in.at[late], tables.at[late])

    def make(src, dst, stage, sem, device):
        return pltpu.make_async_remote_copy(
            src_ref=src, dst_ref=dst, send_sem=sent.at[stage], recv_sem=sem,
            device_id=device, device_id_type=pl.DeviceIdType.MESH,
        )

    def arrived(ref, sem):
        make(ref, ref, 0, sem, {"px": other}).wait_recv()

    def gone(ref, stage):
        make(ref, ref, stage, sems_y.at[0], {"px": other}).wait_send()

    def lines(py):
        return pl.ds(pl.multiple_of(py * rows_y, 8), rows_y)

    three = pl.ds(0, (count_py - 1) * rows_y)

    def row(tile):
        return side * tile + (1 - side) * (rows_x - 1 - tile)

    def fold(replica, chunk):
        span = coming[chunk]
        left = [dens[replica, row(span.start + i)] for i in range(span.size)]
        right = [dens[replica, row(tiles + span.start + i)] for i in range(span.size)]
        both = jnp.concatenate([jnp.concatenate(left, 0), jnp.concatenate(right, 0)], 1)
        waves = matmul(jnp.concatenate(halves(both), 1), table("fold_z"))
        for parity in range(2):
            cut = waves[:, parity * length : (parity + 1) * length]
            a[replica, parity, span] = cut.reshape(span.size, rows_y, length)

    sends_z = {}
    for chunk in range(chunks):
        for step, peer in peers.items():
            replica, parity = role(peer)
            sends_z[step, chunk] = make(
                a.at[replica, parity, coming[chunk]], z.at[coming[chunk], lines(me_py), :],
                0, sems_z.at[chunk], {"py": peer},
            )

    def steps(replica):
        return ((3,), (2, 1)) if replica == 0 else ((2, 1), (3,))

    def scatter(replica, chunk):
        at_outer, at_inner = steps(replica)

        @pl.when(outer)
        def _():
            for step in at_outer:
                sends_z[step, chunk].start()

        @pl.when(jnp.logical_not(outer))
        def _():
            for step in at_inner:
                sends_z[step, chunk].start()

    loads["first"].wait()
    loads["fold_z"].wait()
    for replica in range(replicas):
        if replica == 1:
            loads["rest"].wait()
        for chunk in range(chunks):
            fold(replica, chunk)
            if replica == chunk == 0:
                pl.semaphore_wait(barrier, len(partners))
            scatter(replica, chunk)

    @pl.loop(0, tiles, unroll=4)
    def _(tile):
        z[tile, lines(me_py), :] = a[mine, odd_z, tile]

    def kernel_setup():
        loads["factors"].wait()
        terms = factors.shape[1]
        flat[...] = jnp.zeros_like(flat)
        where = lax.broadcasted_iota(jnp.int32, (terms, length), 1)
        weight = jnp.where(where == 0, 0.5 / length, 1.0 / length)
        for dim in range(3):
            flat[dim, 0:terms] = factors[dim, :, 0:length] * weight
        for dim in range(2):
            turned[dim] = flat[dim].T
        high, low = halves(flat[2])
        gains[...] = jnp.concatenate(
            [jnp.concatenate([high, low], 1), jnp.concatenate([high, jnp.zeros_like(low)], 1)], 0
        )

    def kernel_values(start, count):
        @pl.loop(start, start + count, unroll=8)
        def _(f):
            pair = turned[0] * turned[1, pl.ds(f, 1), :]
            sums = matmul(jnp.concatenate(halves(pair), 1), gains[...])
            kern[f] = sums[:, :length] + sums[:, length:]

    kernel_setup()
    kernel_values(0, half)

    def fold_lines(chunk):
        span = coming[chunk]
        arrived(z.at[span, three, :], sems_z.at[chunk])
        for tile in range(span.start, span.start + span.size, 2):
            width = min(2, span.start + span.size - tile)
            cells = jnp.concatenate([z[tile + j] for j in range(width)], 1)
            waves = matmul(table("fold_y"), jnp.concatenate(halves(cells), 0))
            for parity in range(2):
                for j in range(width):
                    b[parity, tile + j] = waves[
                        parity * half : (parity + 1) * half, j * length : (j + 1) * length
                    ]
        make(b.at[1 - side, span], p.at[span], 1, sems_y.at[chunk], {"px": twin}).start()

    flip = sign.astype(jnp.float32)
    def fold_sheets(chunk):
        span = coming[chunk]
        arrived(p.at[span], sems_y.at[chunk])
        for tile in range(span.start, span.start + span.size):
            ours, theirs = b[side, tile], p[tile]
            total, gap = ours + theirs, (ours - theirs) * flip
            x[part, tile] = jnp.where(core == 0, total, gap)
            swap[tile] = jnp.where(core == 0, gap, total)
        make(swap.at[span], x.at[part, span], 2, sems_c.at[chunk], {"px": other}).start()

    def forward(pieces):
        cells = [x[where, span].reshape(span.size * half, length) for where, span in pieces]
        high, low = halves(jnp.concatenate(cells, 0))
        waves = matmul(jnp.concatenate([high, low, high], 1), table("wide", odd_z))
        tall = table("tall", side)[:, : 3 * half]
        each = [(where, tile) for where, span in pieces for tile in range(span.start, span.start + span.size)]
        found = []
        for i in range(len(each)):
            high, low = halves(waves[i * half : (i + 1) * half])
            found.append(matmul(tall, jnp.concatenate([high, high, low], 0)))
        for both, (where, tile) in zip(found, each):
            for j in range(2):
                first = (where * rows_x + j * tiles + tile) * PITCH
                e[pl.ds(first, length), :] = both[:, j * length : (j + 1) * length]

    def swapped(chunk):
        arrived(swap.at[coming[chunk]], sems_c.at[chunk])

    loads["tables"].wait()
    for stage in range(chunks + LAG):
        if stage < chunks:
            fold_lines(stage)
        if stage < 4:
            kernel_values(half + stage * half // 4, half // 4)
        if stage >= LAG:
            fold_sheets(stage - LAG)
        ready = stage - LAG - 3
        if ready >= 0 and ready % 2 == 0 and ready < chunks - 4:
            some = coming[ready : ready + 2]
            swapped(ready)
            swapped(ready + 1)
            forward([(where, span) for where in (part, 1 - part) for span in some])
    forward([(part, span) for span in coming[-4:]])
    for chunk in range(chunks - 4, chunks - 1):
        swapped(chunk)
    forward([(1 - part, span) for span in coming[-4:-1]])
    swapped(chunks - 1)
    forward([(1 - part, coming[-1])])

    def spectrum(first):
        cells = jnp.concatenate([e[pl.ds(first + i, half, stride=PITCH), :] for i in range(2)], 1)
        high, low = halves(cells)
        return matmul(table("tall", core)[:, : 3 * half], jnp.concatenate([high, high, low], 0))

    def answer_of(first, k):
        cells = matmul(table("back_tall", core), solved[k])
        cells = cells[:half] + cells[half:]
        for i in range(2):
            turned_e[pl.ds(first + i, half, stride=PITCH), :] = cells[:, i * length : (i + 1) * length]

    def solve(first, k, waves):
        product = waves * jnp.concatenate([kern[first], kern[first + 1]], 1)
        solved[k] = jnp.concatenate(halves(product), 0)

    def middle():
        trips = length // (2 * GROUP)
        for k in range(GROUP):
            solve(2 * k, k, spectrum(2 * k))

        @pl.loop(1, trips)
        def _(f):
            for k in range(GROUP):
                first = 2 * (f * GROUP + k)
                waves = spectrum(first)
                answer_of(first - 2 * GROUP, k)
                solve(first, k, waves)

        for k in range(GROUP):
            answer_of(length - 2 * GROUP + 2 * k, k)

    middle()

    def backward(chunk):
        span = going[chunk]
        rows = []
        for where in (1 - part, part):
            for i in range(span.size):
                cells = []
                for j in range(2):
                    start = (where * rows_x + j * tiles + span.start + i) * PITCH
                    cells.append(turned_e[pl.ds(start, length), :])
                cells = jnp.concatenate(halves(jnp.concatenate(cells, 1)), 0)
                cells = matmul(table("back_tall", side), cells)
                rows.append(cells[:half] + cells[half:])
        high, low = halves(jnp.concatenate(rows, 0))
        wide = table("back_wide", odd_z)
        wide = jnp.concatenate([wide[:, :length], wide[:, length:]], 0)
        cells = matmul(jnp.concatenate([high, low, high], 1), wide)
        found = cells.reshape(2, span.size, half, length)
        c_send[span], keep[span] = found[0], found[1]
        make(c_send.at[span], c_held.at[span], 3, sems_ci.at[chunk], {"px": other}).start()

    def open_sheets(chunk):
        span = going[chunk]
        arrived(c_held.at[span], sems_ci.at[chunk])
        for tile in range(span.start, span.start + span.size):
            first, second = keep[tile], c_held[tile]
            even = jnp.where(core == 0, first, second)
            odd = jnp.where(core == 0, second, first) * flip
            g[side, tile] = even + odd
            g_send[tile] = even - odd
        make(g_send.at[span], g.at[side, span], 4, sems_yi.at[chunk], {"px": twin}).start()

    def answer(step, chunk):
        span = going[chunk]
        return make(
            zr.at[span, lines(peers[step]), :], fin.at[mine, odd_z, span],
            5, sems_zi.at[mine * (chunk + 1)], {"py": peers[step]},
        )

    def open_lines(chunk):
        span = going[chunk]
        arrived(g_send.at[span], sems_yi.at[chunk])
        for tile in range(span.start, span.start + span.size, 2):
            width = min(2, span.start + span.size - tile)
            both = [
                jnp.concatenate([g[parity, tile + j] for j in range(width)], 1) for parity in range(2)
            ]
            cells = matmul(table("open_y"), jnp.concatenate(halves(jnp.concatenate(both, 0)), 0))
            for j in range(width):
                zr[tile + j] = cells[:, j * length : (j + 1) * length]
        for step in (3, 2):
            answer(step, chunk).start()

        @pl.when(jnp.logical_not(outer))
        def _():
            answer(1, chunk).start()

        fin[mine, odd_z, span] = zr[span, lines(me_py), :]

    for stage in range(chunks + LAG_BACK + 1):
        if stage < chunks:
            backward(stage)
        if 0 <= stage - 1 < chunks:
            open_sheets(stage - 1)
        if 0 <= stage - LAG_BACK - 1:
            open_lines(stage - LAG_BACK - 1)

    @pl.when(outer)
    def _():
        for chunk in range(chunks):
            answer(1, chunk).start()

    for stage, ref in enumerate((z.at[:, three, :], p, swap, c_send, g_send)):
        gone(ref, stage)

    def collect(replica, span, sem):
        few, many = (outer, inner)[:: 1 - 2 * replica]

        @pl.when(few)
        def _():
            arrived(fin.at[replica, 0, span], sem)

        @pl.when(many)
        def _():
            arrived(fin.at[replica, :, span], sem)

    def finish(replica, chunk):
        span = going[chunk]
        if replica == 1:
            collect(replica, span, sems_zi.at[chunk + 1])
        both = [fin[replica, parity, span].reshape(span.size * rows_y, length) for parity in range(2)]
        cells = matmul(jnp.concatenate(halves(jnp.concatenate(both, 1)), 1), table("open_z"))
        for i in range(span.size):
            cut = cells[i * rows_y : (i + 1) * rows_y]
            out[replica, row(span.start + i)] = cut[:, :length]
            out[replica, row(tiles + span.start + i)] = cut[:, length:]

    collect(0, pl.ds(0, tiles), sems_zi.at[0])
    for replica in range(replicas):
        for chunk in range(chunks):
            if replica == 1 and chunk == chunks - 1:
                gone(zr.at[:, three, :], 5)
            finish(replica, chunk)


def twice(table):
    zero = np.zeros_like(table)
    return np.block([[table, zero], [zero, table]])


def tables_of(length):
    half = length // 2
    angle = (np.arange(length)[:, None] * (2 * np.arange(half) + 1) % (4 * length)) * (math.pi / (2 * length))
    waves = np.stack([np.cos(angle), np.sin(angle)]).astype(np.float32)
    high = waves.astype(jnp.bfloat16).astype(np.float32)
    low = waves - high
    near, far = np.eye(half), np.eye(half)[::-1]
    line = np.block([[far, near], [-far, near]])
    sides = [line[:half].T, line[half:].T]
    fold_z = np.concatenate([twice(side) for side in sides], 1)
    fold_z = np.concatenate([fold_z, fold_z], 0)
    fold_y = np.concatenate([line, line], 1)
    open_y = np.concatenate([line.T, line.T], 1)
    open_z = np.concatenate([twice(side.T) for side in sides], 0)
    open_z = np.concatenate([open_z, open_z], 0)
    wide, tall, back_tall, back_wide = [], [], [], []
    for parity in range(2):
        up, down = high[parity], low[parity]
        wide.append(np.concatenate([twice(up.T), twice(up.T), twice(down.T)], 0))
        tall.append(np.concatenate([up, down, up], 1))
        back_tall.append(np.block([[up.T, up.T], [down.T, np.zeros_like(down.T)]]))
        back_wide.append(np.concatenate([twice(up), twice(up), twice(down)], 0))
    tall = np.concatenate(tall, 0)
    back_wide = [np.concatenate(np.split(one, 2, 0), 1) for one in back_wide]
    found = {
        "fold_z": fold_z, "fold_y": fold_y, "wide": np.concatenate(wide, 0),
        "tall": np.pad(tall, ((0, 0), (0, 2 * length - tall.shape[1]))),
        "back_tall": np.concatenate(back_tall, 0), "back_wide": np.concatenate(back_wide, 0),
        "open_y": open_y, "open_z": open_z,
    }
    return {name: one.astype(np.float32).astype(jnp.bfloat16) for name, one in found.items()}


def layout_of(length):
    found, start = {}, 0
    tables = tables_of(length)
    for name, one in tables.items():
        found[name] = (start, one.shape[0])
        start += one.shape[0]
    return found, np.concatenate(list(tables.values()), 0)


def sector_body(density, kernel_factors):
    replicas, rows_x, rows_y, length = density.shape
    half, tiles = length // 2, rows_x // 2
    chunks = tiles // TILES - 2 + 2 * TILES
    f32, bf16 = jnp.float32, jnp.bfloat16
    dma = pltpu.SemaphoreType.DMA
    sheet = (tiles, half, length)
    given = [
        pltpu.with_memory_space_constraint(array, pltpu.HBM)
        for array in (density, kernel_factors, jnp.asarray(layout_of(length)[1]))
    ]
    return pl.pallas_call(
        sector_kernel,
        out_shape=pltpu.VMEM(density.shape, f32),
        in_specs=[pl.BlockSpec(memory_space=pl.ANY)] * len(given),
        out_specs=pl.BlockSpec(memory_space=pltpu.VMEM),
        scratch_shapes=[pltpu.VMEM(array.shape, array.dtype) for array in given] + [
            pltpu.VMEM((replicas, 2, tiles, rows_y, length), f32),
            pltpu.VMEM((tiles, length, length), f32),
            pltpu.VMEM((2,) + sheet, f32), pltpu.VMEM(sheet, f32), pltpu.VMEM(sheet, f32),
            pltpu.VMEM((2,) + sheet, f32),
            pltpu.VMEM((half * PITCH, length), f32), pltpu.VMEM((half * PITCH, length), f32),
            pltpu.VMEM((length, length, length), f32),
            pltpu.VMEM(sheet, f32), pltpu.VMEM(sheet, f32), pltpu.VMEM(sheet, f32),
            pltpu.VMEM((2,) + sheet, f32), pltpu.VMEM(sheet, f32),
            pltpu.VMEM((tiles, length, length), f32),
            pltpu.VMEM((replicas, 2, tiles, rows_y, length), f32),
            pltpu.VMEM((3, length, length), f32), pltpu.VMEM((2, length, length), f32),
            pltpu.VMEM((2 * length, 2 * length), bf16),
            pltpu.VMEM((GROUP, 2 * length, 2 * length), bf16),
            dma((6,)), dma((chunks,)), dma((chunks,)), dma((chunks,)),
            dma((chunks,)), dma((chunks,)), dma((chunks + 1,)), dma((5,)),
        ],
        compiler_params=pltpu.CompilerParams(
            has_side_effects=True, vmem_limit_bytes=56 * 2**20, collective_id=0
        ),
    )(*given)


def body(density, kernel_factors):
    replicas, rows_x, rows_y, length = density.shape
    count_px, count_py = lax.axis_size("px"), lax.axis_size("py")
    square = count_px == count_py == 2 * replicas == 4
    whole = rows_x * count_px == rows_y * count_py == length == LANES
    if square and whole and kernel_factors.shape[1] <= LANES:
        return sector_body(density, kernel_factors)
    return plain_body(density, kernel_factors)


def solution(mesh):
    placed = (P("rep", "px", "py", None), P())
    return jax.shard_map(
        body, mesh=mesh, in_specs=placed, out_specs=P("rep", "px", "py", None), check_vma=False
    )
```
